256 devices in a mesh: tm: 16 (over y, x), sat: 16 (over z, core).
Axes of the slice: x: 4, y: 4, z: 8, core: 2. Of those that a mesh axis runs over, the one named last changes fastest.
Arguments:
- samples: int32 [2, 32, 8192], P(None, 'tm', 'sat'), may hold values from -1073741824 to 1073741823
- codes: int32 [48, 4092], P('sat'), may hold values from -1 to 1, as said below
- dopplers: int32 [64], replicated, may hold values from -60 to 60
Outputs:
- power: float32 [64, 48, 8192], P('tm', 'sat')
- detection: float32 [48], P('sat')
The draws below stay inside these ranges and needn't reach their ends.
Inputs may be any that keep to these rules, and one draw needn't show every extreme that they name: `codes`: each entry is -1 or 1.
All inputs are finite; a program needn't handle non-finite values.
Results may differ from the reference program's by a relative error of at most 0.0003.
Values sent between devices are 32-bit elements.
A program may use at most 64 MiB of HBM per device.

```python
import math
import jax
import jax.numpy as jnp
from jax import lax

N = 8192
CHIPS = 4092
BLOCK_COUNT = 32
DOPPLER = 64
SATS = 48


def draw_samples(key, part):
    key_raw = jax.random.fold_in(key, 11)
    key_shift = jax.random.fold_in(key, 12)
    raw_words = jax.random.randint(key_raw, (2, BLOCK_COUNT, N), -1073741824, 1073741824, dtype=jnp.int32)
    shifts = jax.random.randint(key_shift, (2, BLOCK_COUNT, 32), 0, 3, dtype=jnp.int32)
    shifts = jnp.repeat(shifts, N // 32, axis=2)
    return jnp.right_shift(raw_words, shifts)


def draw_codes(key, part):
    chip_bits = jax.random.randint(jax.random.fold_in(key, 21), (SATS, CHIPS), 0, 2, dtype=jnp.int32)
    return 2 * chip_bits - 1


def with_ends(entries, stream_key, smallest, top_value):
    spot = [jax.random.randint(jax.random.fold_in(stream_key, axis), (), 0, length) for axis, length in enumerate(entries.shape)]
    main_axis = entries.shape.index(max(entries.shape))
    neighbour = spot[:main_axis] + [(spot[main_axis] + 1) % entries.shape[main_axis]] + spot[main_axis + 1:]
    return entries.at[tuple(spot)].set(smallest).at[tuple(neighbour)].set(top_value)


def setup_inputs(seed: int = 0) -> dict:
    seeds = jax.random.split(jax.random.key(seed), 4)
    return {
        "samples": draw_samples(jax.random.fold_in(seeds[3], 71), 0),
        "codes": draw_codes(jax.random.fold_in(seeds[3], 71), 0),
        "dopplers": with_ends(jax.random.randint(seeds[2], (DOPPLER,), -60, 61), jax.random.fold_in(seeds[2], 1), -60, 60).astype(jnp.int32),
    }


sample_scale = 2.0 ** -29
wrap_count = 32768


def replica_rows(codes):
    offsets = jnp.arange(N, dtype=jnp.int32)
    chip_index = (offsets * CHIPS) // N
    halves = jnp.mod((offsets * (2 * CHIPS)) // N, 2)
    sign_rows = (1 - 2 * halves).astype(jnp.float32)
    return jnp.take(codes, chip_index, axis=1).astype(jnp.float32) * sign_rows[None, :]


def reference(samples, codes, dopplers):
    real_part = samples[0].astype(jnp.float32) * sample_scale
    imag_part = samples[1].astype(jnp.float32) * sample_scale
    received_record = lax.complex(real_part, imag_part)
    spectrum = jnp.conj(jnp.fft.fft(replica_rows(codes), axis=-1))
    offsets = jnp.arange(N, dtype=jnp.int32)

    def one_bin(doppler_bin):
        rotation_angles = jnp.mod(doppler_bin * offsets, wrap_count).astype(jnp.float32) * (2.0 * math.pi / wrap_count)
        doppler_mixer = lax.complex(jnp.cos(rotation_angles), -jnp.sin(rotation_angles))
        wiped_record = jnp.fft.fft(received_record * doppler_mixer[None, :], axis=-1)

        def one_sat(code_spec):
            lagged = jnp.fft.ifft(wiped_record * code_spec[None, :], axis=-1)
            return jnp.sum(jnp.real(lagged) ** 2 + jnp.imag(lagged) ** 2, axis=0)

        return lax.map(one_sat, spectrum)

    power_map = lax.map(one_bin, dopplers) * (1.0 / (N * BLOCK_COUNT))
    average_energy = jnp.sum(real_part * real_part + imag_part * imag_part) / (BLOCK_COUNT * N)
    peak_value = jnp.max(power_map, axis=(0, 2))
    detection = peak_value / jnp.maximum(average_energy, 0.25)
    return (power_map, detection)
```

```python
import functools
import math

import jax
import jax.numpy as jnp
import numpy as np
from jax import lax
from jax.experimental import pallas as pl
from jax.experimental.pallas import tpu as pltpu
from jax.sharding import Mesh
from jax.sharding import PartitionSpec as P

SAT = ("sat_0", "sat_1")
TM = ("tm_0", "tm_1")

OUTER = 64
INNER = 128
LENGTH = OUTER * INNER
CHIPS = 4092
BLOCKS = 32
SAMPLE_SCALE = 2.0**-29
WRAP = 32768
CORR_SCALE = 2.0**-22

f32 = jnp.float32
bf16 = jnp.bfloat16


def np_split(w):
    hi = w.astype(np.float32).astype(bf16)
    lo = (w - hi.astype(np.float64)).astype(np.float32).astype(bf16)
    return hi, lo


def dft_tables():
    i = np.arange(OUTER)
    a = 2 * np.pi * ((i[:, None] * i[None, :]) % OUTER) / OUTER
    c, s = np.cos(a), np.sin(a)

    def left(w):
        hi, lo = np_split(w)
        return np.block([[hi, hi], [lo, np.zeros_like(lo)]])

    j = np.arange(INNER)
    b = 2 * np.pi * ((j[:, None] * j[None, :]) % INNER) / INNER
    ci, si = np.cos(b), np.sin(b)
    t = 2 * np.pi * (i[:, None] * j[None, :]) / LENGTH
    return (
        left(np.block([[c, s], [-s, c]])),
        left(np.block([[c, -s], [s, c]])),
        *np_split(np.block([[ci, -si], [si, ci]])),
        *np_split(np.block([[ci, si], [-si, ci]])),
        np.stack([np.cos(t), np.sin(t)]).astype(np.float32),
    )


def dot(a, b):
    return jnp.dot(a, b, preferred_element_type=f32)


def split(v):
    hi = v.astype(bf16)
    return hi, (v - hi.astype(f32)).astype(bf16)


def outer_dft(left, pairs):
    re = jnp.concatenate([p[0] for p in pairs], 1)
    im = jnp.concatenate([p[1] for p in pairs], 1)
    hi, lo = split(jnp.concatenate([re, im], 0))
    o = dot(left, jnp.concatenate([hi, lo], 0))
    o = o[: 2 * OUTER] + o[2 * OUTER :]
    cut = lambda u: slice(INNER * u, INNER * u + INNER)
    return [(o[:OUTER, cut(u)], o[OUTER:, cut(u)]) for u in range(len(pairs))]


def inner_dft(right_hi, right_lo, pairs):
    hi, lo = split(jnp.concatenate([jnp.concatenate(p, 1) for p in pairs], 0))
    o = dot(hi, right_hi) + dot(lo, right_hi) + dot(hi, right_lo)
    cut = lambda u: slice(OUTER * u, OUTER * u + OUTER)
    return [(o[cut(u), :INNER], o[cut(u), INNER:]) for u in range(len(pairs))]


def search(first, last, rows, *refs):
    refs = list(refs)
    xs, ph = refs[:2]
    refs = refs[2:]
    if first:
        rep = refs.pop(0)
    else:
        old, old_stat, cs = refs[:3]
        refs = refs[3:]
    lf, li, rfh, rfl, rih, ril, tw = refs[:7]
    refs = refs[7:]
    out, stat = refs[:2]
    if first:
        cs = refs[2]
    bins, sats = out.shape[:2]
    tc, ts = tw[0], tw[1]

    def forward(pairs):
        p = outer_dft(lf[...], pairs)
        p = [(r * tc + i * ts, i * tc - r * ts) for r, i in p]
        return inner_dft(rfh[...], rfl[...], p)

    def inverse(pairs):
        p = inner_dft(rih[...], ril[...], pairs)
        p = [(r * tc - i * ts, i * tc + r * ts) for r, i in p]
        return outer_dft(li[...], p)

    zero = jnp.zeros((OUTER, INNER), f32)
    if first:
        for s, (r, i) in enumerate(forward([(rep[s], zero) for s in range(sats)])):
            cs[s, 0] = r * CORR_SCALE
            cs[s, 1] = i * CORR_SCALE
        out[...] = jnp.zeros_like(out)
        energy = zero
    else:
        out[...] = old[...]
        energy = old_stat[0]
    units = [(f, s) for f in range(bins) for s in range(sats)]

    def body(b, energy):
        xr = xs[b, 0].astype(f32) * SAMPLE_SCALE
        xi = xs[b, 1].astype(f32) * SAMPLE_SCALE
        ys = forward(
            [
                (xr * ph[f, 0] + xi * ph[f, 1], xi * ph[f, 0] - xr * ph[f, 1])
                for f in range(bins)
            ]
        )
        zs = []
        for f, s in units:
            (yr, yi), cr, ci = ys[f], cs[s, 0], cs[s, 1]
            zs.append((yr * cr + yi * ci, yi * cr - yr * ci))
        for (f, s), (r, i) in zip(units, inverse(zs)):
            out[f, s] += r * r + i * i
        return energy + (xr * xr + xi * xi)

    energy = lax.fori_loop(0, rows, body, energy)
    stat[0] = energy
    if last:
        mean = jnp.sum(energy) * (1.0 / (BLOCKS * LENGTH))
        floor = jnp.maximum(mean, 0.25)
        for s in range(sats):
            m = out[0, s]
            for f in range(1, bins):
                m = jnp.maximum(m, out[f, s])
            stat[1 + s] = jnp.broadcast_to(jnp.max(m) / floor, (OUTER, INNER))


def search_call(xs, ph, rep, state, tables, last):
    first = state is None
    rows, bins = xs.shape[0], ph.shape[0]
    sats = rep.shape[0]
    vm = pl.BlockSpec(memory_space=pltpu.VMEM)
    args = [xs, ph] + ([rep] if first else list(state)) + list(tables)
    shapes = [
        jax.ShapeDtypeStruct((bins, sats, OUTER, INNER), f32),
        jax.ShapeDtypeStruct((1 + sats if last else 1, OUTER, INNER), f32),
    ]
    if first:
        shapes.append(jax.ShapeDtypeStruct((sats, 2, OUTER, INNER), f32))
    res = pl.pallas_call(
        functools.partial(search, first, last, rows),
        out_shape=tuple(shapes),
        in_specs=[vm] * len(args),
        out_specs=tuple([vm] * len(shapes)),
        compiler_params=pltpu.CompilerParams(vmem_limit_bytes=40 * 2**20),
        cost_estimate=pl.CostEstimate(
            flops=rows * 16 * 8192 * 1000, bytes_accessed=2**20, transcendentals=0
        ),
    )(*args)
    return res[0], res[1], (res[2] if first else state[2])


def peers_max(mine, name_sizes):
    n = math.prod(name_sizes.values())
    names = list(name_sizes)

    def kernel(x, o, land, send, recv):
        me = [lax.axis_index(a) for a in names]
        barrier = pltpu.get_barrier_semaphore()

        def at(k):
            k0, k1 = divmod(k, name_sizes[names[1]])
            return {
                names[0]: lax.rem(me[0] + k0, name_sizes[names[0]]),
                names[1]: lax.rem(me[1] + k1, name_sizes[names[1]]),
            }

        for k in range(1, n):
            pl.semaphore_signal(
                barrier, inc=1, device_id=at(k), device_id_type=pl.DeviceIdType.MESH
            )
        pl.semaphore_wait(barrier, n - 1)
        copies = []
        for k in range(1, n):
            copy = pltpu.make_async_remote_copy(
                src_ref=x,
                dst_ref=land.at[k],
                send_sem=send.at[k],
                recv_sem=recv.at[k],
                device_id=at(k),
                device_id_type=pl.DeviceIdType.MESH,
            )
            copy.start()
            copies.append(copy)
        m = x[...]
        for k, copy in enumerate(copies, 1):
            copy.wait_recv()
            m = jnp.maximum(m, land[k])
        for copy in copies:
            copy.wait_send()
        o[...] = m

    vm = pl.BlockSpec(memory_space=pltpu.VMEM)
    return pl.pallas_call(
        kernel,
        out_shape=jax.ShapeDtypeStruct(mine.shape, f32),
        in_specs=[vm],
        out_specs=vm,
        scratch_shapes=[
            pltpu.VMEM((n,) + mine.shape, f32),
            pltpu.SemaphoreType.DMA((n,)),
            pltpu.SemaphoreType.DMA((n,)),
        ],
        compiler_params=pltpu.CompilerParams(collective_id=3, has_side_effects=True),
    )(mine)


def replica_rows(codes):
    sats, chips = codes.shape
    assert (chips, LENGTH) == (CHIPS, 8192)
    c = codes.reshape(sats, 4, 1023).astype(bf16)
    even = jnp.concatenate([c[..., :1], c], -1)
    odd = jnp.concatenate([c[..., :512], c[..., 511:]], -1)
    h = np.arange(1024)
    even = even * np.where((h > 0) & (h <= 512), -1, 1).astype(bf16)
    odd = odd * np.where(h >= 512, -1, 1).astype(bf16)
    spread = np.zeros((2, INNER, 2 * INNER), bf16)
    j = np.arange(INNER)
    spread[0, j, 2 * j] = 1
    spread[1, j, 2 * j + 1] = 1
    rows = dot(even.reshape(-1, INNER), spread[0]) + dot(odd.reshape(-1, INNER), spread[1])
    return rows.reshape(sats, OUTER, INNER)


def phasors(bins):
    n = jnp.arange(LENGTH, dtype=jnp.int32)
    angle = jnp.mod(bins[:, None] * n[None, :], WRAP).astype(f32) * (2.0 * math.pi / WRAP)
    both = jnp.stack([jnp.cos(angle), jnp.sin(angle)], 1)
    return both.reshape(-1, 2, OUTER, INNER)


def shards(samples, codes, dopplers):
    sat_n = lax.axis_size(SAT)
    tm_n = [lax.axis_size(a) for a in TM]
    tables = [jnp.asarray(t) for t in dft_tables()]
    parts = lax.all_to_all(
        jnp.broadcast_to(samples, (sat_n, *samples.shape)), SAT, 0, 0, tiled=True
    )
    parts = parts.reshape(sat_n, 2, samples.shape[1], OUTER // sat_n, INNER)
    own = jnp.transpose(parts, (2, 1, 0, 3, 4)).reshape(samples.shape[1], 2, OUTER, INNER)

    bins = dopplers.shape[0] // math.prod(tm_n)
    row = lax.axis_index(TM)
    ph = phasors(lax.dynamic_slice(dopplers, (row * bins,), (bins,)))
    rep = replica_rows(codes)

    def moved(dy, dx):
        pairs = []
        for y in range(tm_n[0]):
            for x in range(tm_n[1]):
                to = ((y + dy) % tm_n[0]) * tm_n[1] + (x + dx) % tm_n[1]
                pairs.append((y * tm_n[1] + x, to))
        return lax.ppermute(own, TM, pairs)

    groups = [
        [(0, 1), (0, 3), (1, 0), (3, 0)],
        [(1, 1), (1, 3), (3, 1), (3, 3), (0, 2), (2, 0)],
        [(2, 1), (2, 3), (1, 2), (3, 2), (2, 2)],
    ]
    arrivals = [[moved(*o) for o in g] for g in groups]
    state = search_call(own, ph, rep, None, tables, False)
    for k, got in enumerate(arrivals):
        state = search_call(
            jnp.concatenate(got, 0), ph, rep, state, tables, k == len(arrivals) - 1
        )
    power, stat, _ = state
    sats = rep.shape[0]
    peak = peers_max(
        jnp.concatenate([stat[1:, 0], jnp.zeros((8 - sats, INNER), f32)], 0),
        dict(zip(TM, tm_n)),
    )
    return power.reshape(bins, sats, LENGTH), peak[:sats, 0]


def solution(mesh):
    torus = Mesh(mesh.devices.reshape(4, 4, 8, 2), (*TM, *SAT))
    return jax.shard_map(
        shards,
        mesh=torus,
        in_specs=(P(None, TM, SAT), P(SAT, None), P()),
        out_specs=(P(TM, SAT, None), P(SAT)),
        check_vma=False,
    )
```

```python
import functools
import math

import jax
import jax.numpy as jnp
import numpy as np
from jax import lax
from jax.experimental import pallas as pl
from jax.experimental.pallas import tpu as pltpu
from jax.sharding import Mesh
from jax.sharding import PartitionSpec as P

SAT = ("sat_0", "sat_1")
TM = ("tm_0", "tm_1")
MESH_ID = pl.DeviceIdType.MESH

OUTER = 64
INNER = 128
LENGTH = OUTER * INNER
CHIPS = 4092
BLOCKS = 32
SAMPLE_SCALE = 2.0**-29
WRAP = 32768
CORR_SCALE = 2.0**-22

f32 = jnp.float32
bf16 = jnp.bfloat16


def np_split(w):
    hi = w.astype(np.float32).astype(bf16)
    lo = (w - hi.astype(np.float64)).astype(np.float32).astype(bf16)
    return hi, lo


def halves(t):
    return np.stack([t[:, :INNER], t[:, INNER:]])


def dft_tables():
    i = np.arange(OUTER)
    a = 2 * np.pi * ((i[:, None] * i[None, :]) % OUTER) / OUTER
    c, s = np.cos(a), np.sin(a)
    rows = np.concatenate([k + np.arange(8 * b, 8 * b + 8) for b in range(8) for k in (0, 64)])
    cols = np.concatenate(
        [k + np.arange(16 * b, 16 * b + 16) for b in range(4) for k in (0, 128, 64, 192)]
    )

    def left(w):
        hi, lo = np_split(w)
        top = np.block([hi, hi])[rows]
        low = np.block([lo, np.zeros_like(lo)])[rows]
        return halves(np.concatenate([top, low])[:, cols])

    j = np.arange(INNER)
    b = 2 * np.pi * ((j[:, None] * j[None, :]) % INNER) / INNER
    ci, si = np.cos(b), np.sin(b)
    right = [np.block([[ci, -si], [si, ci]]), np.block([[ci, si], [-si, ci]])]
    t = 2 * np.pi * (i[:, None] * j[None, :]) / LENGTH
    return (
        left(np.block([[c, s], [-s, c]])),
        left(np.block([[c, -s], [s, c]])),
        *[halves(m) for r in right for m in np_split(r)],
        np.stack([np.cos(t), np.sin(t)]).astype(np.float32),
    )


def split(v):
    hi = v.astype(bf16)
    return hi, (v - hi.astype(f32)).astype(bf16)


def wide(ref, a, b):
    return jnp.concatenate([ref[0, a:b, :], ref[1, a:b, :]], 1)


def search(xs, ph, rep, lf, li, rfh, rfl, rih, ril, tw, out, stat, cs, ys, zs):
    blocks = xs.shape[0]
    sats, bins = out.shape[:2]
    assert (sats, bins) == (6, 4)
    kinds = []
    for q in range(2):
        kinds += [pltpu.ACC(q)((OUTER, 256), f32)] * 12 + [pltpu.ACC(q)((128, 256), f32)] * 2

    def run(*accs):
        lag_acc = [accs[0:12], accs[14:26]]
        pair_acc = [accs[12:14], accs[26:28]]

        def tile(pairs):
            pieces = []
            for c in range(4):
                got = [[split(v[16 * c : 16 * c + 16]) for v in p] for p in pairs]
                for part in range(2):
                    for prec in range(2):
                        pieces.append(jnp.concatenate([g[part][prec] for g in got], 1))
            return jnp.concatenate(pieces, 0)

        def outer_start(q, k, left, pairs):
            pltpu.matmul_push_rhs(tile(pairs), 0, q)
            pltpu.matmul_acc_lhs(pair_acc[q][k], wide(left, 0, 128), load_staged_rhs=0)
            pltpu.matmul_acc_lhs(pair_acc[q][k], wide(left, 128, 256))

        def outer_end(q, k):
            o = pltpu.matmul_pop(pair_acc[q][k])
            got = []
            for u in range(2):
                v = o[:, INNER * u : INNER * u + INNER]
                got.append(
                    tuple(
                        jnp.concatenate([v[16 * c + d : 16 * c + d + 8] for c in range(8)], 0)
                        for d in (0, 8)
                    )
                )
            return got

        def forward_inner(q):
            tc, ts = tw[0], tw[1]
            v = [
                jnp.concatenate([r * tc + i * ts, i * tc - r * ts], 1)
                for r, i in outer_end(q, 0)
            ]
            hi, lo = split(jnp.concatenate(v, 0))
            pltpu.matmul_push_rhs(wide(rfh, 0, 256), 1, q)
            pltpu.matmul_acc_lhs(pair_acc[q][1], hi, load_staged_rhs=1)
            pltpu.matmul_acc_lhs(pair_acc[q][1], lo)
            pltpu.matmul_push_rhs(wide(rfl, 0, 256), 0, q)
            pltpu.matmul_acc_lhs(pair_acc[q][1], hi, load_staged_rhs=0)

        def forward_end(q):
            o = pltpu.matmul_pop(pair_acc[q][1])
            return [(o[64 * j : 64 * j + 64, :128], o[64 * j : 64 * j + 64, 128:]) for j in range(2)]

        zero = jnp.zeros((OUTER, INNER), f32)
        for base in (0, 2):
            use = [[base + 2 * q, base + 2 * q + 1] for q in range(2)]
            for q in range(2):
                outer_start(q, 0, lf, [(rep[s], zero) for s in use[q]])
            for q in range(2):
                forward_inner(q)
            for q in range(2):
                for s, (r, i) in zip(use[q], forward_end(q)):
                    cs[s, 0] = r * CORR_SCALE
                    cs[s, 1] = i * CORR_SCALE
        out[...] = jnp.zeros_like(out)

        def forward_outer(b):
            xr = xs[b, 0].astype(f32) * SAMPLE_SCALE
            xi = xs[b, 1].astype(f32) * SAMPLE_SCALE
            for q in range(2):
                turned = []
                for f in (2 * q, 2 * q + 1):
                    c, s = ph[f, 0], ph[f, 1]
                    turned.append((xr * c + xi * s, xi * c - xr * s))
                outer_start(q, 0, lf, turned)
            return xr * xr + xi * xi

        def forward_store(slot):
            for q in range(2):
                for j, (r, i) in enumerate(forward_end(q)):
                    ys[slot, 2 * q + j, 0] = r
                    ys[slot, 2 * q + j, 1] = i

        def inverse_inner(slot, batch):
            for q in range(2):
                pltpu.matmul_push_rhs(wide(rih, 0, 256), 1, q)
            for s in range(sats):
                for q in range(2):
                    f = 2 * q + batch
                    yr, yi = ys[slot, f, 0], ys[slot, f, 1]
                    cr, ci = cs[s, 0], cs[s, 1]
                    hi, lo = split(jnp.concatenate([yr * cr + yi * ci, yi * cr - yr * ci], 1))
                    zs[q, s, 0] = hi[:, :128]
                    zs[q, s, 1] = hi[:, 128:]
                    acc = lag_acc[q][batch * 6 + s]
                    pltpu.matmul_acc_lhs(acc, hi, load_staged_rhs=1 if s == 0 else None)
                    pltpu.matmul_acc_lhs(acc, lo)
            for q in range(2):
                pltpu.matmul_push_rhs(wide(ril, 0, 256), 0, q)
            for s in range(sats):
                for q in range(2):
                    pltpu.matmul_acc_lhs(
                        lag_acc[q][batch * 6 + s],
                        wide(zs.at[q, s], 0, OUTER),
                        load_staged_rhs=0 if s == 0 else None,
                    )

        def inverse_outer(batch, p, k):
            tc, ts = tw[0], tw[1]
            for q in range(2):
                pairs = []
                for j in range(2):
                    o = pltpu.matmul_pop(lag_acc[q][batch * 6 + 2 * p + j])
                    r, i = o[:, :128], o[:, 128:]
                    pairs.append((r * tc - i * ts, i * tc + r * ts))
                outer_start(q, k, li, pairs)

        def inverse_power(batch, p, k):
            for q in range(2):
                for j, (r, i) in enumerate(outer_end(q, k)):
                    out[2 * p + j, 2 * q + batch] += r * r + i * i

        def forward_all(b):
            energy = forward_outer(b)
            for q in range(2):
                forward_inner(q)
            return energy

        energy = forward_all(0)
        forward_store(0)

        def body(b, energy):
            slot = lax.rem(b, 2)
            later = forward_outer(jnp.minimum(b + 1, blocks - 1))
            inverse_inner(slot, 0)
            for q in range(2):
                forward_inner(q)
            inverse_inner(slot, 1)
            forward_store(1 - slot)
            steps = [(batch, p) for batch in range(2) for p in range(3)]
            for n, (batch, p) in enumerate(steps):
                inverse_outer(batch, p, n % 2)
                if n:
                    inverse_power(*steps[n - 1], (n - 1) % 2)
            inverse_power(*steps[-1], (len(steps) - 1) % 2)
            return energy + jnp.where(b + 1 < blocks, later, 0.0)

        energy = lax.fori_loop(0, blocks, body, energy)
        stat[...] = jnp.broadcast_to(jnp.sum(energy), (8, INNER))

    pl.run_scoped(run, *kinds)


VM = pl.BlockSpec(memory_space=pltpu.VMEM)


def search_call(xs, ph, rep):
    bins, sats = ph.shape[0], rep.shape[0]
    tables = [jnp.asarray(t) for t in dft_tables()]
    return pl.pallas_call(
        search,
        out_shape=(
            jax.ShapeDtypeStruct((sats, bins, OUTER, INNER), f32),
            jax.ShapeDtypeStruct((8, INNER), f32),
        ),
        in_specs=[VM] * (3 + len(tables)),
        out_specs=(VM, VM),
        scratch_shapes=[
            pltpu.VMEM((sats, 2, OUTER, INNER), f32),
            pltpu.VMEM((2, bins, 2, OUTER, INNER), f32),
            pltpu.VMEM((2, sats, 2, OUTER, INNER), bf16),
        ],
        compiler_params=pltpu.CompilerParams(
            vmem_limit_bytes=32 * 2**20
        ),
    )(xs, ph, rep, *tables)


class Copies:
    def __init__(self, send, recv):
        self.send, self.recv, self.made = send, recv, {}

    def start(self, key, src, dst, to):
        n = len(self.made)
        copy = pltpu.make_async_remote_copy(
            src_ref=src,
            dst_ref=dst,
            send_sem=self.send.at[n],
            recv_sem=self.recv.at[n],
            device_id=to,
            device_id_type=MESH_ID,
        )
        self.made[key] = copy
        copy.start()

    def arrive(self, key):
        self.made[key].wait_recv()

    def drain(self):
        for copy in self.made.values():
            copy.wait_send()


def greet(targets):
    barrier = pltpu.get_barrier_semaphore()
    for to in targets:
        pl.semaphore_signal(barrier, inc=1, device_id=to, device_id_type=MESH_ID)
    pl.semaphore_wait(barrier, len(targets))


def gather(sizes, x, rep, xs, reps, send, recv, local):
    y, xx, z, core = (lax.axis_index(a) for a in (*TM, *SAT))
    ny, nx, nz, nc = (sizes[a] for a in (*TM, *SAT))
    sat, sat_n = z * nc + core, nz * nc
    tm = y * nx + xx
    move = lambda axis, at, by: {axis: lax.rem(at + by + sizes[axis], sizes[axis])}
    peers = []
    for k in range(1, sat_n):
        t = lax.rem(sat + k, sat_n)
        peers.append((t % nc, {SAT[0]: t // nc, SAT[1]: t % nc}))
    near = [move(TM[0], y, 1), move(TM[0], y, -1), move(TM[1], xx, 1), move(TM[1], xx, -1)]
    greet([to for _, to in peers] + near)

    copies = Copies(send, recv)
    for k, (block, to) in enumerate(peers):
        copies.start(("sat", k), x.at[:, block], xs.at[tm, :, sat], to)
    other = {SAT[1]: 1 - core}
    copies.start("rep", rep, reps.at[1], other)
    mine = [
        pltpu.make_async_copy(x.at[:, core], xs.at[tm, :, sat], local.at[0]),
        pltpu.make_async_copy(rep, reps.at[0], local.at[1]),
    ]
    for c in mine:
        c.start()
    for c in mine:
        c.wait()
    for k in range(len(peers)):
        copies.arrive(("sat", k))

    ways = []
    for h in range(2):
        a_name, b_name = (TM[1], TM[0]) if h == 0 else (TM[0], TM[1])
        a, b = (xx, y) if h == 0 else (y, xx)
        na, nb = sizes[a_name], sizes[b_name]

        def piece(da, db, part, h=h, a=a, b=b, na=na, nb=nb):
            pa, pb = lax.rem(a + da + na, na), lax.rem(b + db + nb, nb)
            slot = pb * nx + pa if h == 0 else pa * nx + pb
            ref = xs.at[slot, h]
            half = sat_n // 2
            return {0: ref, 1: ref.at[0:half], 2: ref.at[half:sat_n]}[part]

        to = {
            "A+": move(a_name, a, 1),
            "A-": move(a_name, a, -1),
            "B+": move(b_name, b, 1),
            "B-": move(b_name, b, -1),
        }
        ways.append((h, piece, to))

    def go(way, name, da, db, part):
        h, piece, to = way
        ref = piece(da, db, part)
        copies.start((h, name, da, db, part), ref, ref, to[name])

    def got(way, name, da, db, part):
        copies.arrive((way[0], name, da, db, part))

    for way in ways:
        for name in ("A+", "A-", "B+", "B-"):
            go(way, name, 0, 0, 0)
    for way in ways:
        got(way, "A+", 0, 0, 0)
        go(way, "A+", -1, 0, 1)
        go(way, "B+", -1, 0, 0)
        go(way, "B-", -1, 0, 0)
        got(way, "A-", 0, 0, 0)
        go(way, "A-", 1, 0, 2)
        go(way, "B+", 1, 0, 0)
        go(way, "B-", 1, 0, 0)
    for da in (0, -1, 1):
        for way in ways:
            got(way, "B+", da, 0, 0)
            go(way, "B+", da, -1, 1)
            got(way, "B-", da, 0, 0)
            go(way, "B-", da, 1, 2)
        if da == 0:
            for way in ways:
                got(way, "A+", -1, 0, 1)
                for name in ("B+", "B-"):
                    go(way, name, 2, 0, 1)
                got(way, "A-", 1, 0, 2)
                for name in ("B+", "B-"):
                    go(way, name, 2, 0, 2)
    for way in ways:
        got(way, "B+", 2, 0, 1)
        go(way, "B+", 2, -1, 1)
        got(way, "B-", 2, 0, 1)
        got(way, "B+", 2, 0, 2)
        got(way, "B-", 2, 0, 2)
        go(way, "B-", 2, 1, 2)
    for way in ways:
        for da in (0, -1, 1, 2):
            got(way, "B+", da, -1, 1)
            got(way, "B-", da, 1, 2)
    copies.arrive("rep")
    copies.drain()


def gather_call(x, rep, sizes):
    tm_n = sizes[TM[0]] * sizes[TM[1]]
    sat_n = sizes[SAT[0]] * sizes[SAT[1]]
    sems = sat_n + 44
    return pl.pallas_call(
        functools.partial(gather, sizes),
        out_shape=(
            jax.ShapeDtypeStruct((tm_n, 2, sat_n, *x.shape[2:]), x.dtype),
            jax.ShapeDtypeStruct((2, *rep.shape), rep.dtype),
        ),
        in_specs=[VM, VM],
        out_specs=(VM, VM),
        scratch_shapes=[
            pltpu.SemaphoreType.DMA((sems,)),
            pltpu.SemaphoreType.DMA((sems,)),
            pltpu.SemaphoreType.DMA((2,)),
        ],
        compiler_params=pltpu.CompilerParams(
            collective_id=1, has_side_effects=True, vmem_limit_bytes=16 * 2**20
        ),
    )(x, rep)


def finish(sizes, part, stat, out, det, land, land_stat, peak, land_peak, send, recv):
    y, xx, core = (lax.axis_index(a) for a in (*TM, SAT[1]))
    ny, nx = sizes[TM[0]], sizes[TM[1]]
    tm, tm_n = y * nx + xx, ny * nx
    sats, bins = land.shape[:2]
    other = {SAT[1]: 1 - core}
    peers = []
    for k in range(1, tm_n):
        t = lax.rem(tm + k, tm_n)
        peers.append({TM[0]: t // nx, TM[1]: t % nx})
    greet([other] + peers)
    copies = Copies(send, recv)
    for s in range(sats):
        copies.start(("part", s), part.at[sats + s], land.at[s], other)
    copies.start("stat", stat, land_stat, other)
    tops = []
    for s in range(sats):
        copies.arrive(("part", s))
        top = None
        for f in range(bins):
            v = part[s, f] + land[s, f]
            out[s, pl.ds(f, OUTER, stride=bins), :] = v
            top = v if top is None else jnp.maximum(top, v)
        tops.append(jnp.broadcast_to(jnp.max(top), (1, INNER)))
    tops += [jnp.zeros((8 - sats, INNER), f32)]
    mine = jnp.concatenate(tops, 0)
    peak[...] = mine
    copies.arrive("stat")
    mean = (stat[...] + land_stat[...]) * (1.0 / (BLOCKS * LENGTH))
    for k, to in enumerate(peers):
        copies.start(("peak", k), peak, land_peak.at[k], to)
    for k in range(len(peers)):
        copies.arrive(("peak", k))
        mine = jnp.maximum(mine, land_peak[k])
    det[...] = mine / jnp.maximum(mean, 0.25)
    copies.drain()


def finish_call(part, stat, sizes):
    sats, bins = part.shape[0] // 2, part.shape[1]
    tm_n = sizes[TM[0]] * sizes[TM[1]]
    sems = sats + tm_n
    return pl.pallas_call(
        functools.partial(finish, sizes),
        out_shape=(
            jax.ShapeDtypeStruct((sats, OUTER * bins, INNER), f32),
            jax.ShapeDtypeStruct((8, INNER), f32),
        ),
        in_specs=[VM, VM],
        out_specs=(VM, VM),
        scratch_shapes=[
            pltpu.VMEM((sats, bins, OUTER, INNER), f32),
            pltpu.VMEM((8, INNER), f32),
            pltpu.VMEM((8, INNER), f32),
            pltpu.VMEM((tm_n - 1, 8, INNER), f32),
            pltpu.SemaphoreType.DMA((sems,)),
            pltpu.SemaphoreType.DMA((sems,)),
        ],
        compiler_params=pltpu.CompilerParams(
            collective_id=2, has_side_effects=True, vmem_limit_bytes=16 * 2**20
        ),
    )(part, stat)


def replica_rows(codes):
    sats, chips = codes.shape
    assert (chips, LENGTH) == (CHIPS, 8192)
    c = codes.reshape(sats, 4, 1023).astype(bf16)
    even = jnp.concatenate([c[..., :1], c], -1)
    odd = jnp.concatenate([c[..., :512], c[..., 511:]], -1)
    h = np.arange(1024)
    even = even * np.where((h > 0) & (h <= 512), -1, 1).astype(bf16)
    odd = odd * np.where(h >= 512, -1, 1).astype(bf16)
    spread = np.zeros((2, INNER, 2 * INNER), bf16)
    j = np.arange(INNER)
    spread[0, j, 2 * j] = 1
    spread[1, j, 2 * j + 1] = 1
    dot = functools.partial(jnp.dot, preferred_element_type=f32)
    rows = dot(even.reshape(-1, INNER), spread[0]) + dot(odd.reshape(-1, INNER), spread[1])
    return rows.reshape(sats, OUTER, INNER)


def phasors(bins):
    n = jnp.arange(LENGTH, dtype=jnp.int32)
    angle = jnp.mod(bins[:, None] * n[None, :], WRAP).astype(f32) * (2.0 * math.pi / WRAP)
    both = jnp.stack([jnp.cos(angle), jnp.sin(angle)], 1)
    return both.reshape(-1, 2, OUTER, INNER)


def shards(samples, codes, dopplers):
    sizes = {a: lax.axis_size(a) for a in (*TM, *SAT)}
    tm_n = sizes[TM[0]] * sizes[TM[1]]
    bins = dopplers.shape[0] // tm_n
    sats = codes.shape[0]
    x = samples.reshape(2, samples.shape[1], -1, INNER)
    rep = replica_rows(codes)
    ph = phasors(lax.dynamic_slice(dopplers, (lax.axis_index(TM) * bins,), (bins,)))
    xs, reps = gather_call(x, rep, sizes)
    part, stat = search_call(
        xs.reshape(tm_n, 2, OUTER, INNER), ph, reps.reshape(2 * sats, OUTER, INNER)
    )
    power, det = finish_call(part, stat, sizes)
    power = power.reshape(sats, OUTER, bins, INNER).transpose(2, 0, 1, 3)
    return power.reshape(bins, sats, LENGTH), det[:sats, 0]


def solution(mesh):
    torus = Mesh(mesh.devices.reshape(4, 4, 8, 2), (*TM, *SAT))
    body = jax.shard_map(
        shards,
        mesh=torus,
        in_specs=(P(None, TM, SAT), P(SAT, None), P()),
        out_specs=(P(TM, SAT, None), P(SAT)),
        check_vma=False,
    )
    with jax.sharding.use_abstract_mesh(torus.abstract_mesh):
        return body
```

```python
import functools
import math

import jax
import jax.numpy as jnp
import numpy as np
from jax import lax
from jax.experimental import pallas as pl
from jax.experimental.pallas import tpu as pltpu
from jax.sharding import Mesh
from jax.sharding import PartitionSpec as P

SAT = ("sat_0", "sat_1")
TM = ("tm_0", "tm_1")
MESH_ID = pl.DeviceIdType.MESH

OUTER = 64
INNER = 128
LENGTH = OUTER * INNER
CHIPS = 4092
BLOCKS = 32
SAMPLE_SCALE = 2.0**-29
WRAP = 32768
CORR_SCALE = 2.0**-22

f32 = jnp.float32
bf16 = jnp.bfloat16


def np_split(w):
    hi = w.astype(np.float32).astype(bf16)
    lo = (w - hi.astype(np.float64)).astype(np.float32).astype(bf16)
    return hi, lo


def halves(t):
    return np.stack([t[:, :INNER], t[:, INNER:]])


def dft_tables():
    i = np.arange(OUTER)
    a = 2 * np.pi * ((i[:, None] * i[None, :]) % OUTER) / OUTER
    c, s = np.cos(a), np.sin(a)
    rows = np.concatenate([k + np.arange(8 * b, 8 * b + 8) for b in range(8) for k in (0, 64)])
    cols = np.concatenate(
        [k + np.arange(16 * b, 16 * b + 16) for b in range(4) for k in (0, 128, 64, 192)]
    )

    def left(w):
        hi, lo = np_split(w)
        top = np.block([hi, hi])[rows]
        low = np.block([lo, np.zeros_like(lo)])[rows]
        return halves(np.concatenate([top, low])[:, cols])

    j = np.arange(INNER)
    b = 2 * np.pi * ((j[:, None] * j[None, :]) % INNER) / INNER
    ci, si = np.cos(b), np.sin(b)
    right = [np.block([[ci, -si], [si, ci]]), np.block([[ci, si], [-si, ci]])]
    t = 2 * np.pi * (i[:, None] * j[None, :]) / LENGTH
    return (
        left(np.block([[c, s], [-s, c]])),
        left(np.block([[c, -s], [s, c]])),
        *[halves(m) for r in right for m in np_split(r)],
        np.stack([np.cos(t), np.sin(t)]).astype(np.float32),
    )


def split(v):
    hi = v.astype(bf16)
    return hi, (v - hi.astype(f32)).astype(bf16)


def wide(ref, a, b):
    return jnp.concatenate([ref[0, a:b, :], ref[1, a:b, :]], 1)


def search_kinds():
    kinds = []
    for q in range(2):
        kinds += [pltpu.ACC(q)((OUTER, 256), f32)] * 12 + [pltpu.ACC(q)((128, 256), f32)] * 2
    return kinds


def search(hooks, xs, ph, reps, lf, li, rfh, rfl, rih, ril, tw, out, cs, ys, zs, accs):
    blocks = xs.shape[0]
    sats, bins = out.shape[:2]
    assert (sats, bins) == (6, 4)
    rep = lambda s: reps[s // 3][s % 3]
    if True:
        lag_acc = [accs[0:12], accs[14:26]]
        pair_acc = [accs[12:14], accs[26:28]]

        def tile(pairs):
            pieces = []
            for c in range(4):
                got = [[split(v[16 * c : 16 * c + 16]) for v in p] for p in pairs]
                for part in range(2):
                    for prec in range(2):
                        pieces.append(jnp.concatenate([g[part][prec] for g in got], 1))
            return jnp.concatenate(pieces, 0)

        def outer_start(q, k, left, pairs):
            pltpu.matmul_push_rhs(tile(pairs), 0, q)
            pltpu.matmul_acc_lhs(pair_acc[q][k], wide(left, 0, 128), load_staged_rhs=0)
            pltpu.matmul_acc_lhs(pair_acc[q][k], wide(left, 128, 256))

        def outer_end(q, k):
            o = pltpu.matmul_pop(pair_acc[q][k])
            got = []
            for u in range(2):
                v = o[:, INNER * u : INNER * u + INNER]
                got.append(
                    tuple(
                        jnp.concatenate([v[16 * c + d : 16 * c + d + 8] for c in range(8)], 0)
                        for d in (0, 8)
                    )
                )
            return got

        def forward_inner(q):
            tc, ts = tw[0], tw[1]
            v = [
                jnp.concatenate([r * tc + i * ts, i * tc - r * ts], 1)
                for r, i in outer_end(q, 0)
            ]
            hi, lo = split(jnp.concatenate(v, 0))
            pltpu.matmul_push_rhs(wide(rfh, 0, 256), 1, q)
            pltpu.matmul_acc_lhs(pair_acc[q][1], hi, load_staged_rhs=1)
            pltpu.matmul_acc_lhs(pair_acc[q][1], lo)
            pltpu.matmul_push_rhs(wide(rfl, 0, 256), 0, q)
            pltpu.matmul_acc_lhs(pair_acc[q][1], hi, load_staged_rhs=0)

        def forward_end(q):
            o = pltpu.matmul_pop(pair_acc[q][1])
            return [(o[64 * j : 64 * j + 64, :128], o[64 * j : 64 * j + 64, 128:]) for j in range(2)]

        hooks["codes"]()
        zero = jnp.zeros((OUTER, INNER), f32)
        for base in (0, 2):
            use = [[base + 2 * q, base + 2 * q + 1] for q in range(2)]
            for q in range(2):
                outer_start(q, 0, lf, [(rep(s), zero) for s in use[q]])
            for q in range(2):
                forward_inner(q)
            for q in range(2):
                for s, (r, i) in zip(use[q], forward_end(q)):
                    cs[s, 0] = r * CORR_SCALE
                    cs[s, 1] = i * CORR_SCALE
        out[...] = jnp.zeros_like(out)

        def forward_outer(b):
            xr, xi = (
                xs[b, h].reshape(OUTER, INNER).astype(f32) * SAMPLE_SCALE for h in range(2)
            )
            for q in range(2):
                turned = []
                for f in (2 * q, 2 * q + 1):
                    c, s = ph[f, 0], ph[f, 1]
                    turned.append((xr * c + xi * s, xi * c - xr * s))
                outer_start(q, 0, lf, turned)
            return xr * xr + xi * xi

        def forward_store(slot):
            for q in range(2):
                for j, (r, i) in enumerate(forward_end(q)):
                    ys[slot, 2 * q + j, 0] = r
                    ys[slot, 2 * q + j, 1] = i

        def inverse_inner(slot, batch):
            for q in range(2):
                pltpu.matmul_push_rhs(wide(rih, 0, 256), 1, q)
            for s in range(sats):
                for q in range(2):
                    f = 2 * q + batch
                    yr, yi = ys[slot, f, 0], ys[slot, f, 1]
                    cr, ci = cs[s, 0], cs[s, 1]
                    hi, lo = split(jnp.concatenate([yr * cr + yi * ci, yi * cr - yr * ci], 1))
                    zs[q, s, 0] = hi[:, :128]
                    zs[q, s, 1] = hi[:, 128:]
                    acc = lag_acc[q][batch * 6 + s]
                    pltpu.matmul_acc_lhs(acc, hi, load_staged_rhs=1 if s == 0 else None)
                    pltpu.matmul_acc_lhs(acc, lo)
            for q in range(2):
                pltpu.matmul_push_rhs(wide(ril, 0, 256), 0, q)
            for s in range(sats):
                for q in range(2):
                    pltpu.matmul_acc_lhs(
                        lag_acc[q][batch * 6 + s],
                        wide(zs.at[q, s], 0, OUTER),
                        load_staged_rhs=0 if s == 0 else None,
                    )

        def inverse_outer(batch, p, k):
            tc, ts = tw[0], tw[1]
            for q in range(2):
                pairs = []
                for j in range(2):
                    o = pltpu.matmul_pop(lag_acc[q][batch * 6 + 2 * p + j])
                    r, i = o[:, :128], o[:, 128:]
                    pairs.append((r * tc - i * ts, i * tc + r * ts))
                outer_start(q, k, li, pairs)

        def inverse_power(batch, p, k):
            for q in range(2):
                for j, (r, i) in enumerate(outer_end(q, k)):
                    out[2 * p + j, 2 * q + batch] += r * r + i * i

        def forward_all(b):
            energy = forward_outer(b)
            for q in range(2):
                forward_inner(q)
            return energy

        hooks["own"]()
        energy = forward_all(0)
        forward_store(0)

        def body(b, energy):
            for k, stage in enumerate(hooks["stages"]):
                pl.when(b == k)(stage)
            slot = lax.rem(b, 2)
            later = forward_outer(jnp.minimum(b + 1, blocks - 1))
            inverse_inner(slot, 0)
            for q in range(2):
                forward_inner(q)
            inverse_inner(slot, 1)
            forward_store(1 - slot)
            steps = [(batch, p) for batch in range(2) for p in range(3)]
            for n, (batch, p) in enumerate(steps):
                inverse_outer(batch, p, n % 2)
                if n:
                    inverse_power(*steps[n - 1], (n - 1) % 2)
            inverse_power(*steps[-1], (len(steps) - 1) % 2)
            return energy + jnp.where(b + 1 < blocks, later, 0.0)

        return lax.fori_loop(0, blocks, body, energy)


VM = pl.BlockSpec(memory_space=pltpu.VMEM)


class Copies:
    def __init__(self, send, recv):
        self.send, self.recv, self.made = send, recv, {}

    def make(self, key):
        n, src, dst, to = self.made[key]
        return pltpu.make_async_remote_copy(
            src_ref=src(),
            dst_ref=dst(),
            send_sem=self.send.at[n],
            recv_sem=self.recv.at[n],
            device_id=to,
            device_id_type=MESH_ID,
        )

    def start(self, key, src, dst, to):
        self.made[key] = (len(self.made), src, dst, to)
        self.make(key).start()

    def arrive(self, key):
        self.make(key).wait_recv()

    def drain(self):
        for key in self.made:
            self.make(key).wait_send()


def greet(targets):
    barrier = pltpu.get_barrier_semaphore()
    for to in targets:
        pl.semaphore_signal(barrier, inc=1, device_id=to, device_id_type=MESH_ID)
    pl.semaphore_wait(barrier, len(targets))


def positions(ny, nx):
    far = lambda d, n: min(d, n - d)
    order = sorted(
        ((dy, dx) for dy in range(ny) for dx in range(nx)),
        key=lambda o: (far(o[0], ny) + far(o[1], nx), max(far(o[0], ny), far(o[1], nx)), o),
    )
    return {o: p for p, o in enumerate(order)}


def whole(sizes, x, rep, ph, *refs):
    tables, refs = refs[:7], refs[7:]
    out, det, xs, rep2, part, cs, ys, zs, land, stat, stat2, peak, peak2, send, recv, local = refs
    y, xx, z, core = (lax.axis_index(a) for a in (*TM, *SAT))
    ny, nx, nz, nc = (sizes[a] for a in (*TM, *SAT))
    sat, sat_n = z * nc + core, nz * nc
    tm, tm_n = y * nx + xx, ny * nx
    sats, bins = land.shape[:2]
    move = lambda axis, at, by: {axis: lax.rem(at + by + sizes[axis], sizes[axis])}
    peers = []
    for k in range(1, sat_n):
        t = lax.rem(sat + k, sat_n)
        peers.append((t % nc, {SAT[0]: t // nc, SAT[1]: t % nc}))
    others = []
    for k in range(1, tm_n):
        t = lax.rem(tm + k, tm_n)
        others.append({TM[0]: t // nx, TM[1]: t % nx})
    partner = {SAT[1]: 1 - core}
    greet([to for _, to in peers] + others)

    copies = Copies(send, recv)
    for k, (block, to) in enumerate(peers):
        copies.start(("sat", k), lambda b=block: x.at[:, b], lambda: xs.at[0, :, sat], to)
    copies.start("rep", lambda: rep, lambda: rep2, partner)
    mine = pltpu.make_async_copy(x.at[:, core], xs.at[0, :, sat], local.at[0])
    mine.start()

    place = positions(ny, nx)
    half = sat_n // 2
    ways = []
    for h in range(2):
        names, at, n = ((TM[1], TM[0]), (xx, y), (nx, ny))
        if h:
            names, at, n = names[::-1], at[::-1], n[::-1]
        to = {}
        for axis in range(2):
            for sign, by in (("+", 1), ("-", -1)):
                to["AB"[axis] + sign] = (axis, by, move(names[axis], at[axis], by))
        ways.append((h, n, to))

    def piece(way, da, db, which):
        h, n, _ = way
        da, db = da % n[0], db % n[1]
        ref = xs.at[place[(da, db) if h else (db, da)], h]
        return {0: ref, 1: ref.at[0:half], 2: ref.at[half:sat_n]}[which]

    def go(way, name, da, db, which):
        axis, by, to = way[2][name]
        there = (da - by, db) if axis == 0 else (da, db - by)
        copies.start(
            (way[0], name, da, db, which),
            lambda: piece(way, da, db, which),
            lambda: piece(way, *there, which),
            to,
        )

    def got(way, name, da, db, which):
        copies.arrive((way[0], name, da, db, which))

    def codes():
        copies.arrive("rep")

    def own():
        mine.wait()
        for k in range(len(peers)):
            copies.arrive(("sat", k))
        for way in ways:
            for name in ("A+", "A-", "B+", "B-"):
                go(way, name, 0, 0, 0)

    def first():
        for way in ways:
            got(way, "A+", 0, 0, 0)
            go(way, "A+", -1, 0, 1)
            got(way, "A-", 0, 0, 0)
            go(way, "A-", 1, 0, 2)
        for way in ways:
            got(way, "B+", 0, 0, 0)
            got(way, "B-", 0, 0, 0)
        for way in ways:
            for da in (-1, 1):
                go(way, "B+", da, 0, 0)
                go(way, "B-", da, 0, 0)
        for way in ways:
            go(way, "B+", 0, -1, 1)
            go(way, "B-", 0, 1, 2)

    def second():
        for way in ways:
            got(way, "A+", -1, 0, 1)
            got(way, "A-", 1, 0, 2)
            for name in ("B+", "B-"):
                go(way, name, 2, 0, 1)
                go(way, name, 2, 0, 2)

    def third():
        for way in ways:
            for da in (-1, 1):
                got(way, "B+", da, 0, 0)
                go(way, "B+", da, -1, 1)
                got(way, "B-", da, 0, 0)
                go(way, "B-", da, 1, 2)

    def fourth():
        for way in ways:
            for which in (1, 2):
                got(way, "B+", 2, 0, which)
                got(way, "B-", 2, 0, which)
            go(way, "B+", 2, -1, 1)
            go(way, "B-", 2, 1, 2)
            for da in (0, -1, 1):
                got(way, "B+", da, -1, 1)
                got(way, "B-", da, 1, 2)

    def fifth():
        for way in ways:
            got(way, "B+", 2, -1, 1)
            got(way, "B-", 2, 1, 2)

    nothing = lambda: None
    hooks = {
        "codes": codes,
        "own": own,
        "stages": [first, second, third, nothing, fourth, nothing, fifth],
    }

    def run(*accs):
        energy = search(hooks, xs, ph, (rep, rep2), *tables, part, cs, ys, zs, accs)
        stat[...] = jnp.broadcast_to(jnp.sum(energy), (8, INNER))

    pl.run_scoped(run, *search_kinds())

    for s in range(sats):
        copies.start(("part", s), lambda s=s: part.at[sats + s], lambda s=s: land.at[s], partner)
    copies.start("stat", lambda: stat, lambda: stat2, partner)
    tops = []
    for s in range(sats):
        copies.arrive(("part", s))
        top = None
        for f in range(bins):
            v = part[s, f] + land[s, f]
            out[s, pl.ds(f, OUTER, stride=bins), :] = v
            top = v if top is None else jnp.maximum(top, v)
        tops.append(jnp.broadcast_to(jnp.max(top), (1, INNER)))
    tops.append(jnp.zeros((8 - sats, INNER), f32))
    copies.arrive("stat")
    mean = (stat[...] + stat2[...]) * (1.0 / (BLOCKS * LENGTH))
    best = jnp.concatenate(tops, 0) / jnp.maximum(mean, 0.25)
    peak[...] = best
    for k, to in enumerate(others):
        copies.start(("peak", k), lambda: peak, lambda k=k: peak2.at[k], to)
    for k in range(len(others)):
        copies.arrive(("peak", k))
        best = jnp.maximum(best, peak2[k])
    det[...] = best
    copies.drain()


def whole_call(x, rep, ph, sizes):
    sats, bins = rep.shape[0], ph.shape[0]
    tm_n = sizes[TM[0]] * sizes[TM[1]]
    sat_n = sizes[SAT[0]] * sizes[SAT[1]]
    tables = [jnp.asarray(t) for t in dft_tables()]
    sems = sat_n + 44 + sats + tm_n
    return pl.pallas_call(
        functools.partial(whole, sizes),
        out_shape=(
            jax.ShapeDtypeStruct((sats, OUTER * bins, INNER), f32),
            jax.ShapeDtypeStruct((8, INNER), f32),
        ),
        in_specs=[VM] * (3 + len(tables)),
        out_specs=(VM, VM),
        scratch_shapes=[
            pltpu.VMEM((tm_n, 2, sat_n, *x.shape[2:]), x.dtype),
            pltpu.VMEM(rep.shape, f32),
            pltpu.VMEM((2 * sats, bins, OUTER, INNER), f32),
            pltpu.VMEM((2 * sats, 2, OUTER, INNER), f32),
            pltpu.VMEM((2, bins, 2, OUTER, INNER), f32),
            pltpu.VMEM((2, 2 * sats, 2, OUTER, INNER), bf16),
            pltpu.VMEM((sats, bins, OUTER, INNER), f32),
            pltpu.VMEM((8, INNER), f32),
            pltpu.VMEM((8, INNER), f32),
            pltpu.VMEM((8, INNER), f32),
            pltpu.VMEM((tm_n - 1, 8, INNER), f32),
            pltpu.SemaphoreType.DMA((sems,)),
            pltpu.SemaphoreType.DMA((sems,)),
            pltpu.SemaphoreType.DMA((1,)),
        ],
        compiler_params=pltpu.CompilerParams(
            collective_id=1,
            has_side_effects=True,
            vmem_limit_bytes=32 * 2**20,
        ),
    )(x, rep, ph, *tables)


def replica_rows(codes):
    sats, chips = codes.shape
    assert (chips, LENGTH) == (CHIPS, 8192)
    c = codes.reshape(sats, 4, 1023).astype(bf16)
    even = jnp.concatenate([c[..., :1], c], -1)
    odd = jnp.concatenate([c[..., :512], c[..., 511:]], -1)
    h = lax.broadcasted_iota(jnp.int32, even.shape, 2)
    even = jnp.where((h > 0) & (h <= 512), -even, even)
    odd = jnp.where(h >= 512, -odd, odd)
    r = lax.broadcasted_iota(jnp.int32, (2 * INNER, 2 * INNER), 0)
    j = lax.broadcasted_iota(jnp.int32, (2 * INNER, 2 * INNER), 1)
    spread = (j == 2 * (r % INNER) + r // INNER).astype(bf16)
    both = jnp.concatenate([even.reshape(-1, INNER), odd.reshape(-1, INNER)], 1)
    rows = jnp.dot(both, spread, preferred_element_type=f32)
    return rows.reshape(sats, OUTER, INNER)


def phasors(bins):
    n = jnp.arange(LENGTH, dtype=jnp.int32)
    angle = jnp.mod(bins[:, None] * n[None, :], WRAP).astype(f32) * (2.0 * math.pi / WRAP)
    both = jnp.stack([jnp.cos(angle), jnp.sin(angle)], 1)
    return both.reshape(-1, 2, OUTER, INNER)


def shards(samples, codes, dopplers):
    sizes = {a: lax.axis_size(a) for a in (*TM, *SAT)}
    tm_n = sizes[TM[0]] * sizes[TM[1]]
    bins = dopplers.shape[0] // tm_n
    sats = codes.shape[0]
    x = samples.reshape(2, samples.shape[1], -1, INNER)
    rep = replica_rows(codes)
    ph = phasors(lax.dynamic_slice(dopplers, (lax.axis_index(TM) * bins,), (bins,)))
    power, det = whole_call(x, rep, ph, sizes)
    power = power.reshape(sats, OUTER, bins, INNER).transpose(2, 0, 1, 3)
    return power.reshape(bins, sats, LENGTH), det[:sats, 0]


def solution(mesh):
    torus = Mesh(mesh.devices.reshape(4, 4, 8, 2), (*TM, *SAT))
    body = jax.shard_map(
        shards,
        mesh=torus,
        in_specs=(P(None, TM, SAT), P(SAT, None), P()),
        out_specs=(P(TM, SAT, None), P(SAT)),
        check_vma=False,
    )
    with jax.sharding.use_abstract_mesh(torus.abstract_mesh):
        return body
```

```python
import functools
import math

import jax
import jax.numpy as jnp
import numpy as np
from jax import lax
from jax.experimental import pallas as pl
from jax.experimental.pallas import tpu as pltpu
from jax.sharding import Mesh
from jax.sharding import PartitionSpec as P

SAT = ("sat_0", "sat_1")
TM = ("tm_0", "tm_1")
MESH_ID = pl.DeviceIdType.MESH

OUTER = 64
INNER = 128
LENGTH = OUTER * INNER
CHIPS = 4092
BLOCKS = 32
SAMPLE_SCALE = 2.0**-29
WRAP = 32768
CORR_SCALE = 2.0**-22

f32 = jnp.float32
bf16 = jnp.bfloat16


def np_split(w):
    hi = w.astype(np.float32).astype(bf16)
    lo = (w - hi.astype(np.float64)).astype(np.float32).astype(bf16)
    return hi, lo


def halves(t):
    return np.stack([t[:, :INNER], t[:, INNER:]])


def dft_tables():
    i = np.arange(OUTER)
    a = 2 * np.pi * ((i[:, None] * i[None, :]) % OUTER) / OUTER
    c, s = np.cos(a), np.sin(a)
    rows = np.concatenate([k + np.arange(8 * b, 8 * b + 8) for b in range(8) for k in (0, 64)])
    cols = np.concatenate(
        [k + np.arange(16 * b, 16 * b + 16) for b in range(4) for k in (0, 128, 64, 192)]
    )

    def left(w):
        hi, lo = np_split(w)
        top = np.block([hi, hi])[rows]
        low = np.block([lo, np.zeros_like(lo)])[rows]
        return halves(np.concatenate([top, low])[:, cols])

    j = np.arange(INNER)
    b = 2 * np.pi * ((j[:, None] * j[None, :]) % INNER) / INNER
    ci, si = np.cos(b), np.sin(b)
    right = [np.block([[ci, -si], [si, ci]]), np.block([[ci, si], [-si, ci]])]
    t = 2 * np.pi * (i[:, None] * j[None, :]) / LENGTH
    return (
        left(np.block([[c, s], [-s, c]])),
        left(np.block([[c, -s], [s, c]])),
        *[halves(m) for r in right for m in np_split(r)],
        np.stack([np.cos(t), np.sin(t)]).astype(np.float32),
    )


def split(v):
    hi = v.astype(bf16)
    return hi, (v - hi.astype(f32)).astype(bf16)


def wide(ref, a, b):
    return jnp.concatenate([ref[0, a:b, :], ref[1, a:b, :]], 1)


def search_kinds():
    kinds = []
    for q in range(2):
        kinds += [pltpu.ACC(q)((OUTER, 256), f32)] * 8 + [pltpu.ACC(q)((128, 256), f32)] * 4
    return kinds


def search(hooks, xs, ph, reps, lf, li, rfh, rfl, rih, ril, tw, out, cs, ys, zs, accs):
    blocks = xs.shape[0]
    sats, bins = out.shape[:2]
    assert (sats, bins) == (6, 4)
    rep = lambda s: reps[s // 3][s % 3]
    if True:
        lag_acc = [accs[0:8], accs[12:20]]
        pair_acc = [accs[8:12], accs[20:24]]

        def tile(pairs):
            pieces = []
            for c in range(4):
                got = [[split(v[16 * c : 16 * c + 16]) for v in p] for p in pairs]
                for part in range(2):
                    for prec in range(2):
                        pieces.append(jnp.concatenate([g[part][prec] for g in got], 1))
            return jnp.concatenate(pieces, 0)

        def outer_start(q, k, left, pairs):
            pltpu.matmul_push_rhs(tile(pairs), 0, q)
            pltpu.matmul_acc_lhs(pair_acc[q][k], wide(left, 0, 128), load_staged_rhs=0)
            pltpu.matmul_acc_lhs(pair_acc[q][k], wide(left, 128, 256))

        def outer_end(q, k):
            o = pltpu.matmul_pop(pair_acc[q][k])
            got = []
            for u in range(2):
                v = o[:, INNER * u : INNER * u + INNER]
                got.append(
                    tuple(
                        jnp.concatenate([v[16 * c + d : 16 * c + d + 8] for c in range(8)], 0)
                        for d in (0, 8)
                    )
                )
            return got

        def forward_inner(q):
            tc, ts = tw[0], tw[1]
            v = [
                jnp.concatenate([r * tc + i * ts, i * tc - r * ts], 1)
                for r, i in outer_end(q, 3)
            ]
            hi, lo = split(jnp.concatenate(v, 0))
            pltpu.matmul_push_rhs(wide(rfh, 0, 256), 1, q)
            pltpu.matmul_acc_lhs(pair_acc[q][3], hi, load_staged_rhs=1)
            pltpu.matmul_acc_lhs(pair_acc[q][3], lo)
            pltpu.matmul_push_rhs(wide(rfl, 0, 256), 0, q)
            pltpu.matmul_acc_lhs(pair_acc[q][3], hi, load_staged_rhs=0)

        def forward_end(q):
            o = pltpu.matmul_pop(pair_acc[q][3])
            return [(o[64 * j : 64 * j + 64, :128], o[64 * j : 64 * j + 64, 128:]) for j in range(2)]

        for acc in accs:
            pltpu.matmul_pop(acc)
        hooks["codes"]()
        zero = jnp.zeros((OUTER, INNER), f32)
        for base in (0, 2):
            use = [[base + 2 * q, base + 2 * q + 1] for q in range(2)]
            for q in range(2):
                outer_start(q, 3, lf, [(rep(s), zero) for s in use[q]])
            for q in range(2):
                forward_inner(q)
            for q in range(2):
                for s, (r, i) in zip(use[q], forward_end(q)):
                    cs[s, 0] = r * CORR_SCALE
                    cs[s, 1] = i * CORR_SCALE
        out[...] = jnp.zeros_like(out)

        def signal(b):
            return [xs[b, h].reshape(OUTER, INNER).astype(f32) * SAMPLE_SCALE for h in range(2)]

        def forward_outer(q, x):
            turned = []
            for f in (2 * q, 2 * q + 1):
                c, s = ph[f, 0], ph[f, 1]
                turned.append((x[0] * c + x[1] * s, x[1] * c - x[0] * s))
            outer_start(q, 3, lf, turned)

        def forward_store(q, slot):
            for j, (r, i) in enumerate(forward_end(q)):
                ys[slot, 2 * q + j, 0] = r
                ys[slot, 2 * q + j, 1] = i

        def unit(u):
            return u % sats, u // sats

        def inverse_inner(q, slot, u):
            s, second = unit(u)
            f = 2 * q + second
            if u % 4 == 0:
                pltpu.matmul_push_rhs(wide(rih, 0, 256), 1, q)
            yr, yi = ys[slot, f, 0], ys[slot, f, 1]
            cr, ci = cs[s, 0], cs[s, 1]
            hi, lo = split(jnp.concatenate([yr * cr + yi * ci, yi * cr - yr * ci], 1))
            zs[q, u % 4, 0] = hi[:, :128]
            zs[q, u % 4, 1] = hi[:, 128:]
            acc = lag_acc[q][u % 8]
            pltpu.matmul_acc_lhs(acc, hi, load_staged_rhs=1 if u % 4 == 0 else None)
            pltpu.matmul_acc_lhs(acc, lo)

        def inverse_inner_low(q, group):
            pltpu.matmul_push_rhs(wide(ril, 0, 256), 0, q)
            for u in range(4 * group, 4 * group + 4):
                pltpu.matmul_acc_lhs(
                    lag_acc[q][u % 8],
                    wide(zs.at[q, u % 4], 0, OUTER),
                    load_staged_rhs=0 if u % 4 == 0 else None,
                )

        def inverse_outer(q, p):
            tc, ts = tw[0], tw[1]
            pairs = []
            for u in (2 * p, 2 * p + 1):
                o = pltpu.matmul_pop(lag_acc[q][u % 8])
                r, i = o[:, :128], o[:, 128:]
                pairs.append((r * tc - i * ts, i * tc + r * ts))
            outer_start(q, p % 3, li, pairs)

        def inverse_power(q, p):
            for u, (r, i) in zip((2 * p, 2 * p + 1), outer_end(q, p % 3)):
                s, second = unit(u)
                out[s, 2 * q + second] += r * r + i * i

        part = functools.partial

        def group_steps(q, slot, group):
            steps = [(64, part(inverse_inner, q, slot, u)) for u in range(4 * group, 4 * group + 4)]
            return steps + [(128, part(inverse_inner_low, q, group))]

        def pair_steps(q, p):
            return [(128, part(inverse_outer, q, p)), (0, part(inverse_power, q, (p - 2) % 6))]

        def early(q, slot, x):
            return [
                (128, part(forward_outer, q, x)),
                *group_steps(q, slot, 0),
                (192, part(forward_inner, q)),
                *group_steps(q, slot, 1),
                *pair_steps(q, 0),
                *pair_steps(q, 1),
            ]

        def late(q, slot):
            return [
                *group_steps(q, slot, 2),
                (0, part(forward_store, q, 1 - slot)),
                *[step for p in range(2, 6) for step in pair_steps(q, p)],
            ]

        def merged(streams):
            at = [0, 0]
            todo = [list(v) for v in streams]
            while any(todo):
                q = min((at[q], q) for q in range(2) if todo[q])[1]
                cost, step = todo[q].pop(0)
                step()
                at[q] += cost

        for f in (2, 3):
            for k in range(2):
                ys[1, f, k] = zero
        hooks["own"]()
        x = signal(0)
        energy = x[0] * x[0] + x[1] * x[1]
        for q in range(2):
            forward_outer(q, x)
        for q in range(2):
            forward_inner(q)
        forward_store(0, 0)

        def body(b, energy):
            for k, stage in enumerate(hooks["stages"]):
                pl.when(b == k)(stage)
            slot = lax.rem(b, 2)
            x = signal(jnp.minimum(b + 1, blocks - 1))
            merged([early(0, slot, x) + late(0, slot), late(1, 1 - slot) + early(1, slot, x)])
            return energy + jnp.where(b + 1 < blocks, x[0] * x[0] + x[1] * x[1], 0.0)

        energy = lax.fori_loop(0, blocks, body, energy)
        merged([[], late(1, (blocks - 1) % 2)])
        for q in range(2):
            for p in (4, 5):
                inverse_power(q, p)
        return energy


VM = pl.BlockSpec(memory_space=pltpu.VMEM)


class Copies:
    def __init__(self, send, recv):
        self.send, self.recv, self.made = send, recv, {}

    def make(self, key):
        n, src, dst, to = self.made[key]
        return pltpu.make_async_remote_copy(
            src_ref=src(),
            dst_ref=dst(),
            send_sem=self.send.at[n],
            recv_sem=self.recv.at[n],
            device_id=to,
            device_id_type=MESH_ID,
        )

    def start(self, key, src, dst, to):
        self.made[key] = (len(self.made), src, dst, to)
        self.make(key).start()

    def arrive(self, key):
        self.make(key).wait_recv()

    def drain(self):
        for key in self.made:
            self.make(key).wait_send()


def phasors(turns, start, ph):
    shape = ph.shape[2:]
    n = lax.broadcasted_iota(jnp.int32, shape, 0) * INNER + lax.broadcasted_iota(jnp.int32, shape, 1)
    for f in range(ph.shape[0]):
        m = (turns[start + f] * n) & (WRAP - 1)
        quarter = (m + WRAP // 8) >> 13
        t = (m - (quarter << 13)).astype(f32) * (2.0 * math.pi / WRAP)
        u = t * t
        sine = t * (1 + u * (-1 / 6 + u * (1 / 120 + u * (-1 / 5040 + u * (1 / 362880)))))
        cosine = 1 + u * (
            -1 / 2 + u * (1 / 24 + u * (-1 / 720 + u * (1 / 40320 + u * (-1 / 3628800))))
        )
        odd, half = (quarter & 1) == 1, (quarter & 2) == 2
        c = jnp.where(odd, -sine, cosine)
        s = jnp.where(odd, cosine, sine)
        ph[f, 0] = jnp.where(half, -c, c)
        ph[f, 1] = jnp.where(half, -s, s)


def positions(ny, nx):
    far = lambda d, n: min(d, n - d)
    order = sorted(
        ((dy, dx) for dy in range(ny) for dx in range(nx)),
        key=lambda o: (far(o[0], ny) + far(o[1], nx), max(far(o[0], ny), far(o[1], nx)), o),
    )
    return {o: p for p, o in enumerate(order)}


def whole(sizes, x, rep, bins_ref, *refs):
    far_tables, out, det, tables, ph, refs = refs[:7], refs[7], refs[8], refs[9:16], refs[16], refs[17:]
    xs, rep2, part, cs, ys, zs, land, stat, stat2, peak, peak2, send, recv, local = refs
    y, xx, z, core = (lax.axis_index(a) for a in (*TM, *SAT))
    ny, nx, nz, nc = (sizes[a] for a in (*TM, *SAT))
    sat, sat_n = z * nc + core, nz * nc
    tm, tm_n = y * nx + xx, ny * nx
    sats, bins = land.shape[:2]
    move = lambda axis, at, by: {axis: lax.rem(at + by + sizes[axis], sizes[axis])}
    peers = []
    for k in range(1, sat_n):
        t = lax.rem(sat + k, sat_n)
        peers.append((t % nc, {SAT[0]: t // nc, SAT[1]: t % nc}))
    others = []
    for k in range(1, tm_n):
        t = lax.rem(tm + k, tm_n)
        others.append({TM[0]: t // nx, TM[1]: t % nx})
    partner = {SAT[1]: 1 - core}
    fetches = [pltpu.make_async_copy(*p, local.at[1 + k]) for k, p in enumerate(zip(far_tables, tables))]
    for fetch in fetches:
        fetch.start()
    barrier = pltpu.get_barrier_semaphore()
    greeted = [to for _, to in peers] + others
    for to in greeted:
        pl.semaphore_signal(barrier, inc=1, device_id=to, device_id_type=MESH_ID)
    phasors(bins_ref, tm * bins, ph)
    pl.semaphore_wait(barrier, len(greeted))

    copies = Copies(send, recv)
    for k, (block, to) in enumerate(peers):
        copies.start(("sat", k), lambda b=block: x.at[:, b], lambda: xs.at[0, :, sat], to)
    copies.start("rep", lambda: rep, lambda: rep2, partner)
    mine = pltpu.make_async_copy(x.at[:, core], xs.at[0, :, sat], local.at[0])
    mine.start()

    place = positions(ny, nx)
    half = sat_n // 2
    ways = []
    for h in range(2):
        names, at, n = ((TM[1], TM[0]), (xx, y), (nx, ny))
        if h:
            names, at, n = names[::-1], at[::-1], n[::-1]
        to = {}
        for axis in range(2):
            for sign, by in (("+", 1), ("-", -1)):
                to["AB"[axis] + sign] = (axis, by, move(names[axis], at[axis], by))
        ways.append((h, n, to))

    def piece(way, da, db, which):
        h, n, _ = way
        da, db = da % n[0], db % n[1]
        ref = xs.at[place[(da, db) if h else (db, da)], h]
        return {0: ref, 1: ref.at[0:half], 2: ref.at[half:sat_n]}[which]

    def go(way, name, da, db, which):
        axis, by, to = way[2][name]
        there = (da - by, db) if axis == 0 else (da, db - by)
        copies.start(
            (way[0], name, da, db, which),
            lambda: piece(way, da, db, which),
            lambda: piece(way, *there, which),
            to,
        )

    def got(way, name, da, db, which):
        copies.arrive((way[0], name, da, db, which))

    def codes():
        for fetch in fetches:
            fetch.wait()
        copies.arrive("rep")

    def own():
        mine.wait()
        for k in range(len(peers)):
            copies.arrive(("sat", k))
        for way in ways:
            for name in ("A+", "A-", "B+", "B-"):
                go(way, name, 0, 0, 0)

    def first():
        for way in ways:
            got(way, "A+", 0, 0, 0)
            go(way, "A+", -1, 0, 1)
            got(way, "A-", 0, 0, 0)
            go(way, "A-", 1, 0, 2)
        for way in ways:
            got(way, "B+", 0, 0, 0)
            got(way, "B-", 0, 0, 0)
        for way in ways:
            for da in (-1, 1):
                go(way, "B+", da, 0, 0)
                go(way, "B-", da, 0, 0)
        for way in ways:
            go(way, "B+", 0, -1, 1)
            go(way, "B-", 0, 1, 2)

    def second():
        for way in ways:
            got(way, "A+", -1, 0, 1)
            got(way, "A-", 1, 0, 2)
            for name in ("B+", "B-"):
                go(way, name, 2, 0, 1)
                go(way, name, 2, 0, 2)

    def third():
        for way in ways:
            for da in (-1, 1):
                got(way, "B+", da, 0, 0)
                go(way, "B+", da, -1, 1)
                got(way, "B-", da, 0, 0)
                go(way, "B-", da, 1, 2)

    def fourth():
        for way in ways:
            for which in (1, 2):
                got(way, "B+", 2, 0, which)
                got(way, "B-", 2, 0, which)
            go(way, "B+", 2, -1, 1)
            go(way, "B-", 2, 1, 2)
            for da in (0, -1, 1):
                got(way, "B+", da, -1, 1)
                got(way, "B-", da, 1, 2)

    def fifth():
        for way in ways:
            got(way, "B+", 2, -1, 1)
            got(way, "B-", 2, 1, 2)

    nothing = lambda: None
    hooks = {
        "codes": codes,
        "own": own,
        "stages": [first, second, third, nothing, fourth, nothing, fifth],
    }

    def run(*accs):
        energy = search(hooks, xs, ph, (rep, rep2), *tables, part, cs, ys, zs, accs)
        stat[...] = jnp.broadcast_to(jnp.sum(energy), (8, INNER))

    pl.run_scoped(run, *search_kinds())

    for s in range(sats):
        copies.start(("part", s), lambda s=s: part.at[sats + s], lambda s=s: land.at[s], partner)
    copies.start("stat", lambda: stat, lambda: stat2, partner)
    tops = []
    for s in range(sats):
        copies.arrive(("part", s))
        top = None
        for f in range(bins):
            v = part[s, f] + land[s, f]
            out[s, pl.ds(f, OUTER, stride=bins), :] = v
            top = v if top is None else jnp.maximum(top, v)
        tops.append(jnp.broadcast_to(jnp.max(top), (1, INNER)))
    tops.append(jnp.zeros((8 - sats, INNER), f32))
    copies.arrive("stat")
    mean = (stat[...] + stat2[...]) * (1.0 / (BLOCKS * LENGTH))
    best = jnp.concatenate(tops, 0) / jnp.maximum(mean, 0.25)
    peak[...] = best
    for k, to in enumerate(others):
        copies.start(("peak", k), lambda: peak, lambda k=k: peak2.at[k], to)
    for k in range(len(others)):
        copies.arrive(("peak", k))
        best = jnp.maximum(best, peak2[k])
    det[...] = best
    copies.drain()


def whole_call(x, rep, turns, sizes):
    sats = rep.shape[0]
    tm_n = sizes[TM[0]] * sizes[TM[1]]
    sat_n = sizes[SAT[0]] * sizes[SAT[1]]
    tables = [jnp.asarray(t) for t in dft_tables()]
    bins = turns.shape[0] // tm_n
    sems = sat_n + 44 + sats + tm_n
    return pl.pallas_call(
        functools.partial(whole, sizes),
        out_shape=(
            jax.ShapeDtypeStruct((sats, OUTER * bins, INNER), f32),
            jax.ShapeDtypeStruct((8, INNER), f32),
        ),
        in_specs=[VM, VM, pl.BlockSpec(memory_space=pltpu.SMEM)]
        + [pl.BlockSpec(memory_space=pltpu.HBM)] * len(tables),
        out_specs=(VM, VM),
        scratch_shapes=[pltpu.VMEM(t.shape, t.dtype) for t in tables]
        + [
            pltpu.VMEM((bins, 2, OUTER, INNER), f32),
            pltpu.VMEM((tm_n, 2, sat_n, *x.shape[2:]), x.dtype),
            pltpu.VMEM(rep.shape, f32),
            pltpu.VMEM((2 * sats, bins, OUTER, INNER), f32),
            pltpu.VMEM((2 * sats, 2, OUTER, INNER), f32),
            pltpu.VMEM((2, bins, 2, OUTER, INNER), f32),
            pltpu.VMEM((2, 4, 2, OUTER, INNER), bf16),
            pltpu.VMEM((sats, bins, OUTER, INNER), f32),
            pltpu.VMEM((8, INNER), f32),
            pltpu.VMEM((8, INNER), f32),
            pltpu.VMEM((8, INNER), f32),
            pltpu.VMEM((tm_n - 1, 8, INNER), f32),
            pltpu.SemaphoreType.DMA((sems,)),
            pltpu.SemaphoreType.DMA((sems,)),
            pltpu.SemaphoreType.DMA((1 + len(tables),)),
        ],
        compiler_params=pltpu.CompilerParams(
            collective_id=1,
            has_side_effects=True,
            vmem_limit_bytes=32 * 2**20,
        ),
    )(x, rep, turns, *tables)


def replica_rows(codes):
    sats, chips = codes.shape
    assert (chips, LENGTH) == (CHIPS, 8192)
    c = codes.reshape(sats, 4, 1023).astype(bf16)
    even = jnp.concatenate([c[..., :1], c], -1)
    odd = jnp.concatenate([c[..., :512], c[..., 511:]], -1)
    h = lax.broadcasted_iota(jnp.int32, even.shape, 2)
    even = jnp.where((h > 0) & (h <= 512), -even, even)
    odd = jnp.where(h >= 512, -odd, odd)
    r = lax.broadcasted_iota(jnp.int32, (2 * INNER, 2 * INNER), 0)
    j = lax.broadcasted_iota(jnp.int32, (2 * INNER, 2 * INNER), 1)
    spread = (j == 2 * (r % INNER) + r // INNER).astype(bf16)
    both = jnp.concatenate([even.reshape(-1, INNER), odd.reshape(-1, INNER)], 1)
    rows = jnp.dot(both, spread, preferred_element_type=f32)
    return rows.reshape(sats, OUTER, INNER)


def shards(samples, codes, dopplers):
    sizes = {a: lax.axis_size(a) for a in (*TM, *SAT)}
    tm_n = sizes[TM[0]] * sizes[TM[1]]
    bins = dopplers.shape[0] // tm_n
    sats = codes.shape[0]
    x = samples.reshape(2, samples.shape[1], -1, INNER)
    rep = replica_rows(codes)
    power, det = whole_call(x, rep, dopplers, sizes)
    power = power.reshape(sats, OUTER, bins, INNER).transpose(2, 0, 1, 3)
    return power.reshape(bins, sats, LENGTH), det[:sats, 0]


def solution(mesh):
    torus = Mesh(mesh.devices.reshape(4, 4, 8, 2), (*TM, *SAT))
    body = jax.shard_map(
        shards,
        mesh=torus,
        in_specs=(P(None, TM, SAT), P(SAT, None), P()),
        out_specs=(P(TM, SAT, None), P(SAT)),
        check_vma=False,
    )
    with jax.sharding.use_abstract_mesh(torus.abstract_mesh):
        return body
```

```python
import functools
import math

import jax
import jax.numpy as jnp
import numpy as np
from jax import lax
from jax.experimental import pallas as pl
from jax.experimental.pallas import tpu as pltpu
from jax.sharding import Mesh
from jax.sharding import PartitionSpec as P

SAT = ("sat_0", "sat_1")
TM = ("tm_0", "tm_1")
MESH_ID = pl.DeviceIdType.MESH

OUTER = 64
INNER = 128
LENGTH = OUTER * INNER
CHIPS = 4092
BLOCKS = 32
SAMPLE_SCALE = 2.0**-29
WRAP = 32768
CORR_SCALE = 2.0**-22

f32 = jnp.float32
bf16 = jnp.bfloat16


def np_split(w):
    hi = w.astype(np.float32).astype(bf16)
    lo = (w - hi.astype(np.float64)).astype(np.float32).astype(bf16)
    return hi, lo


def halves(t):
    return np.stack([t[:, :INNER], t[:, INNER:]])


def dft_tables():
    i = np.arange(OUTER)
    a = 2 * np.pi * ((i[:, None] * i[None, :]) % OUTER) / OUTER
    c, s = np.cos(a), np.sin(a)
    rows = np.concatenate([k + np.arange(8 * b, 8 * b + 8) for b in range(8) for k in (0, 64)])
    cols = np.concatenate(
        [k + np.arange(16 * b, 16 * b + 16) for b in range(4) for k in (0, 128, 64, 192)]
    )

    def left(w):
        hi, lo = np_split(w)
        top = np.block([hi, hi])[rows]
        low = np.block([lo, np.zeros_like(lo)])[rows]
        return halves(np.concatenate([top, low])[:, cols])

    j = np.arange(INNER)
    b = 2 * np.pi * ((j[:, None] * j[None, :]) % INNER) / INNER
    ci, si = np.cos(b), np.sin(b)
    right = [np.block([[ci, -si], [si, ci]]), np.block([[ci, si], [-si, ci]])]
    t = 2 * np.pi * (i[:, None] * j[None, :]) / LENGTH
    return (
        left(np.block([[c, s], [-s, c]])),
        left(np.block([[c, -s], [s, c]])),
        *[halves(m) for r in right for m in np_split(r)],
        np.stack([np.cos(t), np.sin(t)]).astype(np.float32),
    )


def split(v):
    hi = v.astype(bf16)
    return hi, (v - hi.astype(f32)).astype(bf16)


def wide(ref, a, b):
    return jnp.concatenate([ref[0, a:b, :], ref[1, a:b, :]], 1)


def search_kinds():
    kinds = []
    for q in range(2):
        kinds += [pltpu.ACC(q)((OUTER, 256), f32)] * 8 + [pltpu.ACC(q)((128, 256), f32)] * 4
    return kinds


def search(hooks, xs, ph, reps, lf, li, rfh, rfl, rih, ril, tw, out, cs, ys, zs, accs):
    blocks = xs.shape[0]
    sats, bins = out.shape[:2]
    assert (sats, bins) == (6, 4)
    rep = lambda s: reps[s // 3][s % 3]
    if True:
        lag_acc = [accs[0:8], accs[12:20]]
        pair_acc = [accs[8:12], accs[20:24]]

        def tile(pairs):
            pieces = []
            for c in range(4):
                got = [[split(v[16 * c : 16 * c + 16]) for v in p] for p in pairs]
                for part in range(2):
                    for prec in range(2):
                        pieces.append(jnp.concatenate([g[part][prec] for g in got], 1))
            return jnp.concatenate(pieces, 0)

        def outer_start(q, k, left, pairs):
            pltpu.matmul_push_rhs(tile(pairs), 0, q)
            pltpu.matmul_acc_lhs(pair_acc[q][k], wide(left, 0, 128), load_staged_rhs=0)
            pltpu.matmul_acc_lhs(pair_acc[q][k], wide(left, 128, 256))

        def outer_end(q, k):
            o = pltpu.matmul_pop(pair_acc[q][k])
            got = []
            for u in range(2):
                v = o[:, INNER * u : INNER * u + INNER]
                got.append(
                    tuple(
                        jnp.concatenate([v[16 * c + d : 16 * c + d + 8] for c in range(8)], 0)
                        for d in (0, 8)
                    )
                )
            return got

        def forward_inner(q):
            tc, ts = tw[0], tw[1]
            v = [
                jnp.concatenate([r * tc + i * ts, i * tc - r * ts], 1)
                for r, i in outer_end(q, 3)
            ]
            hi, lo = split(jnp.concatenate(v, 0))
            pltpu.matmul_push_rhs(wide(rfh, 0, 256), 1, q)
            pltpu.matmul_acc_lhs(pair_acc[q][3], hi, load_staged_rhs=1)
            pltpu.matmul_acc_lhs(pair_acc[q][3], lo)
            pltpu.matmul_push_rhs(wide(rfl, 0, 256), 0, q)
            pltpu.matmul_acc_lhs(pair_acc[q][3], hi, load_staged_rhs=0)

        def forward_end(q):
            o = pltpu.matmul_pop(pair_acc[q][3])
            return [(o[64 * j : 64 * j + 64, :128], o[64 * j : 64 * j + 64, 128:]) for j in range(2)]

        for acc in accs:
            pltpu.matmul_pop(acc)
        hooks["codes"]()
        zero = jnp.zeros((OUTER, INNER), f32)
        for base in (0, 2):
            use = [[base + 2 * q, base + 2 * q + 1] for q in range(2)]
            for q in range(2):
                outer_start(q, 3, lf, [(rep(s), zero) for s in use[q]])
            for q in range(2):
                forward_inner(q)
            for q in range(2):
                for s, (r, i) in zip(use[q], forward_end(q)):
                    cs[s, 0] = r * CORR_SCALE
                    cs[s, 1] = i * CORR_SCALE
        out[...] = jnp.zeros_like(out)

        def signal(b):
            return [xs[b, h].reshape(OUTER, INNER).astype(f32) * SAMPLE_SCALE for h in range(2)]

        def forward_outer(q, x):
            turned = []
            for f in (2 * q, 2 * q + 1):
                c, s = ph[f, 0], ph[f, 1]
                turned.append((x[0] * c + x[1] * s, x[1] * c - x[0] * s))
            outer_start(q, 3, lf, turned)

        def forward_store(q, slot):
            for j, (r, i) in enumerate(forward_end(q)):
                ys[slot, 2 * q + j, 0] = r
                ys[slot, 2 * q + j, 1] = i

        def unit(u):
            return u % sats, u // sats

        def inverse_inner(q, slot, u):
            s, second = unit(u)
            f = 2 * q + second
            if u % 4 == 0:
                pltpu.matmul_push_rhs(wide(rih, 0, 256), 1, q)
            yr, yi = ys[slot, f, 0], ys[slot, f, 1]
            cr, ci = cs[s, 0], cs[s, 1]
            hi, lo = split(jnp.concatenate([yr * cr + yi * ci, yi * cr - yr * ci], 1))
            zs[q, u % 4, 0] = hi[:, :128]
            zs[q, u % 4, 1] = hi[:, 128:]
            acc = lag_acc[q][u % 8]
            pltpu.matmul_acc_lhs(acc, hi, load_staged_rhs=1 if u % 4 == 0 else None)
            pltpu.matmul_acc_lhs(acc, lo)

        def inverse_inner_low(q, group):
            pltpu.matmul_push_rhs(wide(ril, 0, 256), 0, q)
            for u in range(4 * group, 4 * group + 4):
                pltpu.matmul_acc_lhs(
                    lag_acc[q][u % 8],
                    wide(zs.at[q, u % 4], 0, OUTER),
                    load_staged_rhs=0 if u % 4 == 0 else None,
                )

        def inverse_outer(q, p):
            tc, ts = tw[0], tw[1]
            pairs = []
            for u in (2 * p, 2 * p + 1):
                o = pltpu.matmul_pop(lag_acc[q][u % 8])
                r, i = o[:, :128], o[:, 128:]
                pairs.append((r * tc - i * ts, i * tc + r * ts))
            outer_start(q, p % 3, li, pairs)

        def inverse_power(q, p):
            for u, (r, i) in zip((2 * p, 2 * p + 1), outer_end(q, p % 3)):
                s, second = unit(u)
                out[s, 2 * q + second] += r * r + i * i

        part = functools.partial

        def group_steps(q, slot, group):
            steps = [(64, part(inverse_inner, q, slot, u)) for u in range(4 * group, 4 * group + 4)]
            return steps + [(128, part(inverse_inner_low, q, group))]

        def pair_steps(q, p):
            return [(128, part(inverse_outer, q, p)), (0, part(inverse_power, q, (p - 2) % 6))]

        def early(q, slot, x):
            return [
                (128, part(forward_outer, q, x)),
                *group_steps(q, slot, 0),
                (192, part(forward_inner, q)),
                *group_steps(q, slot, 1),
                *pair_steps(q, 0),
                *pair_steps(q, 1),
            ]

        def late(q, slot):
            return [
                *group_steps(q, slot, 2),
                (0, part(forward_store, q, 1 - slot)),
                *[step for p in range(2, 6) for step in pair_steps(q, p)],
            ]

        def merged(streams):
            at = [0, 0]
            todo = [list(v) for v in streams]
            while any(todo):
                q = min((at[q], q) for q in range(2) if todo[q])[1]
                cost, step = todo[q].pop(0)
                step()
                at[q] += cost

        for f in (2, 3):
            for k in range(2):
                ys[1, f, k] = zero
        hooks["own"]()
        x = signal(0)
        energy = x[0] * x[0] + x[1] * x[1]
        for q in range(2):
            forward_outer(q, x)
        for q in range(2):
            forward_inner(q)
        forward_store(0, 0)

        def body(b, energy):
            for k, stage in hooks["stages"].items():
                pl.when(b == k)(stage)
            slot = lax.rem(b, 2)
            x = signal(jnp.minimum(b + 1, blocks - 1))
            merged([early(0, slot, x) + late(0, slot), late(1, 1 - slot) + early(1, slot, x)])
            return energy + jnp.where(b + 1 < blocks, x[0] * x[0] + x[1] * x[1], 0.0)

        energy = lax.fori_loop(0, blocks, body, energy)
        merged([[], late(1, (blocks - 1) % 2)])
        for q in range(2):
            for p in (4, 5):
                inverse_power(q, p)
        return energy


VM = pl.BlockSpec(memory_space=pltpu.VMEM)


class Copies:
    def __init__(self, send, recv):
        self.send, self.recv, self.made = send, recv, {}

    def make(self, key):
        n, src, dst, to = self.made[key]
        return pltpu.make_async_remote_copy(
            src_ref=src(),
            dst_ref=dst(),
            send_sem=self.send.at[n],
            recv_sem=self.recv.at[n],
            device_id=to,
            device_id_type=MESH_ID,
        )

    def start(self, key, src, dst, to):
        self.made[key] = (len(self.made), src, dst, to)
        self.make(key).start()

    def arrive(self, key):
        self.make(key).wait_recv()

    def drain(self):
        for key in self.made:
            self.make(key).wait_send()


def phasors(turns, start, ph):
    shape = ph.shape[2:]
    n = lax.broadcasted_iota(jnp.int32, shape, 0) * INNER + lax.broadcasted_iota(jnp.int32, shape, 1)
    for f in range(ph.shape[0]):
        m = (turns[start + f] * n) & (WRAP - 1)
        quarter = (m + WRAP // 8) >> 13
        t = (m - (quarter << 13)).astype(f32) * (2.0 * math.pi / WRAP)
        u = t * t
        sine = t * (1 + u * (-1 / 6 + u * (1 / 120 + u * (-1 / 5040 + u * (1 / 362880)))))
        cosine = 1 + u * (
            -1 / 2 + u * (1 / 24 + u * (-1 / 720 + u * (1 / 40320 + u * (-1 / 3628800))))
        )
        odd, half = (quarter & 1) == 1, (quarter & 2) == 2
        c = jnp.where(odd, -sine, cosine)
        s = jnp.where(odd, cosine, sine)
        ph[f, 0] = jnp.where(half, -c, c)
        ph[f, 1] = jnp.where(half, -s, s)


def positions(ny, nx):
    far = lambda d, n: min(d, n - d)
    order = sorted(
        ((dy, dx) for dy in range(ny) for dx in range(nx)),
        key=lambda o: (far(o[0], ny) + far(o[1], nx), max(far(o[0], ny), far(o[1], nx)), o),
    )
    return {o: p for p, o in enumerate(order)}


def whole(sizes, x, rep, bins_ref, *refs):
    tables, out, det, ph, refs = refs[:7], refs[7], refs[8], refs[9], refs[10:]
    xs, rep2, part, cs, ys, zs, land, stat, stat2, peak, peak2, send, recv, local = refs
    y, xx, z, core = (lax.axis_index(a) for a in (*TM, *SAT))
    ny, nx, nz, nc = (sizes[a] for a in (*TM, *SAT))
    sat, sat_n = z * nc + core, nz * nc
    tm, tm_n = y * nx + xx, ny * nx
    sats, bins = land.shape[:2]
    move = lambda axis, at, by: {axis: lax.rem(at + by + sizes[axis], sizes[axis])}
    peers = []
    for k in sorted(range(1, sat_n), key=lambda k: -min(k, sat_n - k)):
        t = lax.rem(sat + k, sat_n)
        peers.append((t % nc, {SAT[0]: t // nc, SAT[1]: t % nc}))
    others = []
    ring = lambda d, n: min(d, n - d)
    for dy, dx in sorted(
        ((dy, dx) for dy in range(ny) for dx in range(nx) if dy or dx),
        key=lambda o: (-ring(o[0], ny) - ring(o[1], nx), o),
    ):
        others.append({**move(TM[0], y, dy), **move(TM[1], xx, dx)})
    partner = {SAT[1]: 1 - core}
    barrier = pltpu.get_barrier_semaphore()
    greeted = [to for _, to in peers] + others
    for to in greeted:
        pl.semaphore_signal(barrier, inc=1, device_id=to, device_id_type=MESH_ID)
    phasors(bins_ref, tm * bins, ph)
    pl.semaphore_wait(barrier, len(greeted))

    copies = Copies(send, recv)
    for k, (block, to) in enumerate(peers):
        copies.start(("sat", k), lambda b=block: x.at[:, b], lambda: xs.at[0, :, sat], to)
    copies.start("rep", lambda: rep, lambda: rep2, partner)
    mine = pltpu.make_async_copy(x.at[:, core], xs.at[0, :, sat], local.at[0])
    mine.start()

    place = positions(ny, nx)
    half = sat_n // 2
    ways = []
    for h in range(2):
        names, at, n = ((TM[1], TM[0]), (xx, y), (nx, ny))
        if h:
            names, at, n = names[::-1], at[::-1], n[::-1]
        to = {}
        for axis in range(2):
            for sign, by in (("+", 1), ("-", -1)):
                to["AB"[axis] + sign] = (axis, by, move(names[axis], at[axis], by))
        ways.append((h, n, to))

    def piece(way, da, db, which):
        h, n, _ = way
        da, db = da % n[0], db % n[1]
        ref = xs.at[place[(da, db) if h else (db, da)], h]
        return {0: ref, 1: ref.at[0:half], 2: ref.at[half:sat_n]}[which]

    def go(way, name, da, db, which):
        axis, by, to = way[2][name]
        there = (da - by, db) if axis == 0 else (da, db - by)
        copies.start(
            (way[0], name, da, db, which),
            lambda: piece(way, da, db, which),
            lambda: piece(way, *there, which),
            to,
        )

    def got(way, name, da, db, which):
        copies.arrive((way[0], name, da, db, which))

    def codes():
        copies.arrive("rep")

    def own():
        mine.wait()
        for k in range(len(peers)):
            copies.arrive(("sat", k))
        for way in ways:
            for name in ("A+", "A-", "B+", "B-"):
                go(way, name, 0, 0, 0)

    def first():
        for way in ways:
            got(way, "A+", 0, 0, 0)
            go(way, "A+", -1, 0, 1)
            got(way, "A-", 0, 0, 0)
            go(way, "A-", 1, 0, 2)
        for way in ways:
            got(way, "B+", 0, 0, 0)
            got(way, "B-", 0, 0, 0)
        for way in ways:
            for da in (-1, 1):
                go(way, "B+", da, 0, 0)
                go(way, "B-", da, 0, 0)
        for way in ways:
            go(way, "B+", 0, -1, 1)
            go(way, "B-", 0, 1, 2)

    def second():
        for way in ways:
            got(way, "A+", -1, 0, 1)
            got(way, "A-", 1, 0, 2)
            for name in ("B+", "B-"):
                go(way, name, 2, 0, 1)
                go(way, name, 2, 0, 2)

    def third():
        for way in ways:
            for da in (-1, 1):
                got(way, "B+", da, 0, 0)
                go(way, "B+", da, -1, 1)
                got(way, "B-", da, 0, 0)
                go(way, "B-", da, 1, 2)

    def fourth():
        for way in ways:
            for which in (1, 2):
                got(way, "B+", 2, 0, which)
                got(way, "B-", 2, 0, which)
            go(way, "B+", 2, -1, 1)
            go(way, "B-", 2, 1, 2)
            for da in (0, -1, 1):
                got(way, "B+", da, -1, 1)
                got(way, "B-", da, 1, 2)

    def fifth():
        for way in ways:
            got(way, "B+", 2, -1, 1)
            got(way, "B-", 2, 1, 2)

    hooks = {
        "codes": codes,
        "own": own,
        "stages": {0: first, 2: second, 4: third, 7: fourth, 10: fifth},
    }

    def run(*accs):
        energy = search(hooks, xs, ph, (rep, rep2), *tables, part, cs, ys, zs, accs)
        stat[...] = jnp.broadcast_to(jnp.sum(energy), (8, INNER))

    pl.run_scoped(run, *search_kinds())

    for s in range(sats):
        copies.start(("part", s), lambda s=s: part.at[sats + s], lambda s=s: land.at[s], partner)
    copies.start("stat", lambda: stat, lambda: stat2, partner)
    tops = []
    for s in range(sats):
        copies.arrive(("part", s))
        top = None
        for f in range(bins):
            v = part[s, f] + land[s, f]
            out[s, pl.ds(f, OUTER, stride=bins), :] = v
            top = v if top is None else jnp.maximum(top, v)
        tops.append(jnp.broadcast_to(jnp.max(top), (1, INNER)))
    tops.append(jnp.zeros((8 - sats, INNER), f32))
    copies.arrive("stat")
    mean = (stat[...] + stat2[...]) * (1.0 / (BLOCKS * LENGTH))
    best = jnp.concatenate(tops, 0) / jnp.maximum(mean, 0.25)
    peak[...] = best
    for k, to in enumerate(others):
        copies.start(("peak", k), lambda: peak, lambda k=k: peak2.at[k], to)
    for k in range(len(others)):
        copies.arrive(("peak", k))
        best = jnp.maximum(best, peak2[k])
    det[...] = best
    copies.drain()


def whole_call(x, rep, turns, sizes):
    sats = rep.shape[0]
    tm_n = sizes[TM[0]] * sizes[TM[1]]
    sat_n = sizes[SAT[0]] * sizes[SAT[1]]
    tables = [jnp.asarray(t) for t in dft_tables()]
    bins = turns.shape[0] // tm_n
    sems = sat_n + 44 + sats + tm_n
    return pl.pallas_call(
        functools.partial(whole, sizes),
        out_shape=(
            jax.ShapeDtypeStruct((sats, OUTER * bins, INNER), f32),
            jax.ShapeDtypeStruct((8, INNER), f32),
        ),
        in_specs=[VM, VM, pl.BlockSpec(memory_space=pltpu.SMEM)]
        + [VM] * len(tables),
        out_specs=(VM, VM),
        scratch_shapes=[
            pltpu.VMEM((bins, 2, OUTER, INNER), f32),
            pltpu.VMEM((tm_n, 2, sat_n, *x.shape[2:]), x.dtype),
            pltpu.VMEM(rep.shape, f32),
            pltpu.VMEM((2 * sats, bins, OUTER, INNER), f32),
            pltpu.VMEM((2 * sats, 2, OUTER, INNER), f32),
            pltpu.VMEM((2, bins, 2, OUTER, INNER), f32),
            pltpu.VMEM((2, 4, 2, OUTER, INNER), bf16),
            pltpu.VMEM((sats, bins, OUTER, INNER), f32),
            pltpu.VMEM((8, INNER), f32),
            pltpu.VMEM((8, INNER), f32),
            pltpu.VMEM((8, INNER), f32),
            pltpu.VMEM((tm_n - 1, 8, INNER), f32),
            pltpu.SemaphoreType.DMA((sems,)),
            pltpu.SemaphoreType.DMA((sems,)),
            pltpu.SemaphoreType.DMA((1,)),
        ],
        compiler_params=pltpu.CompilerParams(
            collective_id=1,
            has_side_effects=True,
            vmem_limit_bytes=32 * 2**20,
        ),
    )(x, rep, turns, *tables)


def replica_rows(codes):
    sats, chips = codes.shape
    assert (chips, LENGTH) == (CHIPS, 8192)
    c = codes.reshape(sats, 4, 1023).astype(bf16)
    even = jnp.concatenate([c[..., :1], c], -1)
    odd = jnp.concatenate([c[..., :512], c[..., 511:]], -1)
    h = lax.broadcasted_iota(jnp.int32, even.shape, 2)
    even = jnp.where((h > 0) & (h <= 512), -even, even)
    odd = jnp.where(h >= 512, -odd, odd)
    r = lax.broadcasted_iota(jnp.int32, (2 * INNER, 2 * INNER), 0)
    j = lax.broadcasted_iota(jnp.int32, (2 * INNER, 2 * INNER), 1)
    spread = (j == 2 * (r % INNER) + r // INNER).astype(bf16)
    both = jnp.concatenate([even.reshape(-1, INNER), odd.reshape(-1, INNER)], 1)
    rows = jnp.dot(both, spread, preferred_element_type=f32)
    return rows.reshape(sats, OUTER, INNER)


def shards(samples, codes, dopplers):
    sizes = {a: lax.axis_size(a) for a in (*TM, *SAT)}
    tm_n = sizes[TM[0]] * sizes[TM[1]]
    bins = dopplers.shape[0] // tm_n
    sats = codes.shape[0]
    x = samples.reshape(2, samples.shape[1], -1, INNER)
    rep = replica_rows(codes)
    power, det = whole_call(x, rep, dopplers, sizes)
    power = power.reshape(sats, OUTER, bins, INNER).transpose(2, 0, 1, 3)
    return power.reshape(bins, sats, LENGTH), det[:sats, 0]


def solution(mesh):
    torus = Mesh(mesh.devices.reshape(4, 4, 8, 2), (*TM, *SAT))
    body = jax.shard_map(
        shards,
        mesh=torus,
        in_specs=(P(None, TM, SAT), P(SAT, None), P()),
        out_specs=(P(TM, SAT, None), P(SAT)),
        check_vma=False,
    )
    with jax.sharding.use_abstract_mesh(torus.abstract_mesh):
        return body
```

```python
import functools
import math

import jax
import jax.numpy as jnp
import numpy as np
from jax import lax
from jax.experimental import pallas as pl
from jax.experimental.pallas import tpu as pltpu
from jax.sharding import Mesh
from jax.sharding import PartitionSpec as P

SAT = ("sat_0", "sat_1")
TM = ("tm_0", "tm_1")
MESH_ID = pl.DeviceIdType.MESH

OUTER = 64
INNER = 128
LENGTH = OUTER * INNER
CHIPS = 4092
BLOCKS = 32
SAMPLE_SCALE = 2.0**-29
WRAP = 32768
CORR_SCALE = 2.0**-22

f32 = jnp.float32
bf16 = jnp.bfloat16


def np_split(w):
    hi = w.astype(np.float32).astype(bf16)
    lo = (w - hi.astype(np.float64)).astype(np.float32).astype(bf16)
    return hi, lo


def halves(t):
    return np.stack([t[:, :INNER], t[:, INNER:]])


def dft_tables():
    i = np.arange(OUTER)
    a = 2 * np.pi * ((i[:, None] * i[None, :]) % OUTER) / OUTER
    c, s = np.cos(a), np.sin(a)
    rows = np.concatenate([k + np.arange(8 * b, 8 * b + 8) for b in range(8) for k in (0, 64)])
    cols = np.concatenate(
        [k + np.arange(16 * b, 16 * b + 16) for b in range(4) for k in (0, 128, 64, 192)]
    )

    def left(w):
        hi, lo = np_split(w)
        top = np.block([hi, hi])[rows]
        low = np.block([lo, np.zeros_like(lo)])[rows]
        return halves(np.concatenate([top, low])[:, cols])

    j = np.arange(INNER)
    b = 2 * np.pi * ((j[:, None] * j[None, :]) % INNER) / INNER
    ci, si = np.cos(b), np.sin(b)
    right = [np.block([[ci, -si], [si, ci]]), np.block([[ci, si], [-si, ci]])]
    t = 2 * np.pi * (i[:, None] * j[None, :]) / LENGTH
    return (
        left(np.block([[c, s], [-s, c]])),
        left(np.block([[c, -s], [s, c]])),
        *[halves(m) for r in right for m in np_split(r)],
        np.stack([np.cos(t), np.sin(t)]).astype(np.float32),
    )


def split(v):
    hi = v.astype(bf16)
    return hi, (v - hi.astype(f32)).astype(bf16)


def wide(ref, a, b):
    return jnp.concatenate([ref[0, a:b, :], ref[1, a:b, :]], 1)


def search_kinds():
    kinds = []
    for q in range(2):
        kinds += [pltpu.ACC(q)((OUTER, 256), f32)] * 8 + [pltpu.ACC(q)((128, 256), f32)] * 4
    return kinds


def search(hooks, xs, ph, reps, lf, li, rfh, rfl, rih, ril, tw, out, cs, ys, zs, accs):
    blocks = xs.shape[0]
    sats, bins = out.shape[:2]
    assert (sats, bins) == (6, 4)
    rep = lambda s: reps[s // 3][s % 3]
    if True:
        lag_acc = [accs[0:8], accs[12:20]]
        pair_acc = [accs[8:12], accs[20:24]]

        def tile(pairs):
            pieces = []
            for c in range(4):
                got = [[split(v[16 * c : 16 * c + 16]) for v in p] for p in pairs]
                for part in range(2):
                    for prec in range(2):
                        pieces.append(jnp.concatenate([g[part][prec] for g in got], 1))
            return jnp.concatenate(pieces, 0)

        def outer_start(q, k, left, pairs):
            pltpu.matmul_push_rhs(tile(pairs), 0, q)
            pltpu.matmul_acc_lhs(pair_acc[q][k], wide(left, 0, 128), load_staged_rhs=0)
            pltpu.matmul_acc_lhs(pair_acc[q][k], wide(left, 128, 256))

        def outer_end(q, k):
            o = pltpu.matmul_pop(pair_acc[q][k])
            got = []
            for u in range(2):
                v = o[:, INNER * u : INNER * u + INNER]
                got.append(
                    tuple(
                        jnp.concatenate([v[16 * c + d : 16 * c + d + 8] for c in range(8)], 0)
                        for d in (0, 8)
                    )
                )
            return got

        def forward_inner(q):
            tc, ts = tw[0], tw[1]
            v = [
                jnp.concatenate([r * tc + i * ts, i * tc - r * ts], 1)
                for r, i in outer_end(q, 3)
            ]
            hi, lo = split(jnp.concatenate(v, 0))
            pltpu.matmul_push_rhs(wide(rfh, 0, 256), 1, q)
            pltpu.matmul_acc_lhs(pair_acc[q][3], hi, load_staged_rhs=1)
            pltpu.matmul_acc_lhs(pair_acc[q][3], lo)
            pltpu.matmul_push_rhs(wide(rfl, 0, 256), 0, q)
            pltpu.matmul_acc_lhs(pair_acc[q][3], hi, load_staged_rhs=0)

        def forward_end(q):
            o = pltpu.matmul_pop(pair_acc[q][3])
            return [(o[64 * j : 64 * j + 64, :128], o[64 * j : 64 * j + 64, 128:]) for j in range(2)]

        for acc in accs:
            pltpu.matmul_pop(acc)
        hooks["codes"]()
        zero = jnp.zeros((OUTER, INNER), f32)
        for base in (0, 2):
            use = [[base + 2 * q, base + 2 * q + 1] for q in range(2)]
            for q in range(2):
                outer_start(q, 3, lf, [(rep(s), zero) for s in use[q]])
            for q in range(2):
                forward_inner(q)
            for q in range(2):
                for s, (r, i) in zip(use[q], forward_end(q)):
                    cs[s, 0] = r * CORR_SCALE
                    cs[s, 1] = i * CORR_SCALE
        out[...] = jnp.zeros_like(out)

        def signal(b):
            return [xs[b, h].reshape(OUTER, INNER).astype(f32) * SAMPLE_SCALE for h in range(2)]

        def forward_outer(q, x):
            turned = []
            for f in (2 * q, 2 * q + 1):
                c, s = ph[f, 0], ph[f, 1]
                turned.append((x[0] * c + x[1] * s, x[1] * c - x[0] * s))
            outer_start(q, 3, lf, turned)

        def forward_store(q, slot):
            for j, (r, i) in enumerate(forward_end(q)):
                ys[slot, 2 * q + j, 0] = r
                ys[slot, 2 * q + j, 1] = i

        def unit(u):
            return u % sats, u // sats

        def inverse_inner(q, slot, u):
            s, second = unit(u)
            f = 2 * q + second
            if u % 4 == 0:
                pltpu.matmul_push_rhs(wide(rih, 0, 256), 1, q)
            yr, yi = ys[slot, f, 0], ys[slot, f, 1]
            cr, ci = cs[s, 0], cs[s, 1]
            hi, lo = split(jnp.concatenate([yr * cr + yi * ci, yi * cr - yr * ci], 1))
            zs[q, u % 4, 0] = hi[:, :128]
            zs[q, u % 4, 1] = hi[:, 128:]
            acc = lag_acc[q][u % 8]
            pltpu.matmul_acc_lhs(acc, hi, load_staged_rhs=1 if u % 4 == 0 else None)
            pltpu.matmul_acc_lhs(acc, lo)

        def inverse_inner_low(q, group):
            pltpu.matmul_push_rhs(wide(ril, 0, 256), 0, q)
            for u in range(4 * group, 4 * group + 4):
                pltpu.matmul_acc_lhs(
                    lag_acc[q][u % 8],
                    wide(zs.at[q, u % 4], 0, OUTER),
                    load_staged_rhs=0 if u % 4 == 0 else None,
                )

        def inverse_outer(q, p):
            tc, ts = tw[0], tw[1]
            pairs = []
            for u in (2 * p, 2 * p + 1):
                o = pltpu.matmul_pop(lag_acc[q][u % 8])
                r, i = o[:, :128], o[:, 128:]
                pairs.append((r * tc - i * ts, i * tc + r * ts))
            outer_start(q, p % 3, li, pairs)

        def inverse_power(q, p):
            for u, (r, i) in zip((2 * p, 2 * p + 1), outer_end(q, p % 3)):
                s, second = unit(u)
                out[s, 2 * q + second] += r * r + i * i

        part = functools.partial

        def group_steps(q, slot, group):
            steps = [(64, part(inverse_inner, q, slot, u)) for u in range(4 * group, 4 * group + 4)]
            return steps + [(128, part(inverse_inner_low, q, group))]

        def pair_steps(q, p):
            return [(128, part(inverse_outer, q, p)), (0, part(inverse_power, q, (p - 2) % 6))]

        def early(q, slot, x):
            ahead = x is not None
            return [
                *([(128, part(forward_outer, q, x))] if ahead else []),
                *group_steps(q, slot, 0),
                *([(192, part(forward_inner, q))] if ahead else []),
                *group_steps(q, slot, 1),
                *pair_steps(q, 0),
                *pair_steps(q, 1),
            ]

        def late(q, slot, ahead=True):
            return [
                *group_steps(q, slot, 2),
                *([(0, part(forward_store, q, 1 - slot))] if ahead else []),
                *[step for p in range(2, 6) for step in pair_steps(q, p)],
            ]

        def merged(streams):
            at = [0, 0]
            todo = [list(v) for v in streams]
            while any(todo):
                q = min((at[q], q) for q in range(2) if todo[q])[1]
                cost, step = todo[q].pop(0)
                step()
                at[q] += cost

        def forward(b):
            x = signal(b)
            for q in range(2):
                forward_outer(q, x)
            for q in range(2):
                forward_inner(q)
            return x[0] * x[0] + x[1] * x[1]

        hooks["own"]()
        energy = forward(0)
        for q in range(2):
            forward_store(q, 0)
        merged([early(0, 0, None) + late(0, 0, False), early(1, 0, None)])
        hooks["first"]()
        energy = energy + forward(1)
        forward_store(0, 1)

        def body(b, energy):
            for k, stage in hooks["stages"].items():
                pl.when(b == k)(stage)
            slot = lax.rem(b, 2)
            x = signal(jnp.minimum(b + 1, blocks - 1))
            merged([early(0, slot, x) + late(0, slot), late(1, 1 - slot) + early(1, slot, x)])
            return energy + jnp.where(b + 1 < blocks, x[0] * x[0] + x[1] * x[1], 0.0)

        energy = lax.fori_loop(1, blocks, body, energy)
        merged([[], late(1, (blocks - 1) % 2)])
        for q in range(2):
            for p in (4, 5):
                inverse_power(q, p)
        return energy


VM = pl.BlockSpec(memory_space=pltpu.VMEM)


class Copies:
    def __init__(self, send, recv):
        self.send, self.recv, self.made = send, recv, {}

    def make(self, key):
        n, src, dst, to = self.made[key]
        return pltpu.make_async_remote_copy(
            src_ref=src(),
            dst_ref=dst(),
            send_sem=self.send.at[n],
            recv_sem=self.recv.at[n],
            device_id=to,
            device_id_type=MESH_ID,
        )

    def start(self, key, src, dst, to):
        self.made[key] = (len(self.made), src, dst, to)
        self.make(key).start()

    def arrive(self, key):
        self.make(key).wait_recv()

    def drain(self):
        for key in self.made:
            self.make(key).wait_send()


def phasors(turns, start, ph):
    shape = ph.shape[2:]
    n = lax.broadcasted_iota(jnp.int32, shape, 0) * INNER + lax.broadcasted_iota(jnp.int32, shape, 1)
    for f in range(ph.shape[0]):
        m = (turns[start + f] * n) & (WRAP - 1)
        quarter = (m + WRAP // 8) >> 13
        t = (m - (quarter << 13)).astype(f32) * (2.0 * math.pi / WRAP)
        u = t * t
        sine = t * (1 + u * (-1 / 6 + u * (1 / 120 + u * (-1 / 5040 + u * (1 / 362880)))))
        cosine = 1 + u * (
            -1 / 2 + u * (1 / 24 + u * (-1 / 720 + u * (1 / 40320 + u * (-1 / 3628800))))
        )
        odd, half = (quarter & 1) == 1, (quarter & 2) == 2
        c = jnp.where(odd, -sine, cosine)
        s = jnp.where(odd, cosine, sine)
        ph[f, 0] = jnp.where(half, -c, c)
        ph[f, 1] = jnp.where(half, -s, s)


def positions(ny, nx):
    far = lambda d, n: min(d, n - d)
    order = sorted(
        ((dy, dx) for dy in range(ny) for dx in range(nx)),
        key=lambda o: (far(o[0], ny) + far(o[1], nx), max(far(o[0], ny), far(o[1], nx)), o),
    )
    return {o: p for p, o in enumerate(order)}


def whole(sizes, x, rep, bins_ref, *refs):
    tables, out, det, ph, refs = refs[:7], refs[7], refs[8], refs[9], refs[10:]
    xs, rep2, part, cs, ys, zs, land, stat, stat2, peak, peak2, send, recv, local = refs
    y, xx, z, core = (lax.axis_index(a) for a in (*TM, *SAT))
    ny, nx, nz, nc = (sizes[a] for a in (*TM, *SAT))
    sat, sat_n = z * nc + core, nz * nc
    tm, tm_n = y * nx + xx, ny * nx
    sats, bins = land.shape[:2]
    move = lambda axis, at, by: {axis: lax.rem(at + by + sizes[axis], sizes[axis])}
    peers = []
    for k in sorted(range(1, sat_n), key=lambda k: -min(k, sat_n - k)):
        t = lax.rem(sat + k, sat_n)
        peers.append((t % nc, {SAT[0]: t // nc, SAT[1]: t % nc}))
    others = []
    ring = lambda d, n: min(d, n - d)
    for dy, dx in sorted(
        ((dy, dx) for dy in range(ny) for dx in range(nx) if dy or dx),
        key=lambda o: (-ring(o[0], ny) - ring(o[1], nx), o),
    ):
        others.append({**move(TM[0], y, dy), **move(TM[1], xx, dx)})
    partner = {SAT[1]: 1 - core}
    barrier = pltpu.get_barrier_semaphore()
    greeted = [to for _, to in peers] + others
    for to in greeted:
        pl.semaphore_signal(barrier, inc=1, device_id=to, device_id_type=MESH_ID)
    phasors(bins_ref, tm * bins, ph)
    pl.semaphore_wait(barrier, len(greeted))

    copies = Copies(send, recv)
    for k, (block, to) in enumerate(peers):
        copies.start(("sat", k), lambda b=block: x.at[:, b], lambda: xs.at[0, :, sat], to)
    copies.start("rep", lambda: rep, lambda: rep2, partner)
    mine = pltpu.make_async_copy(x.at[:, core], xs.at[0, :, sat], local.at[0])
    mine.start()

    place = positions(ny, nx)
    half = sat_n // 2
    ways = []
    for h in range(2):
        names, at, n = ((TM[1], TM[0]), (xx, y), (nx, ny))
        if h:
            names, at, n = names[::-1], at[::-1], n[::-1]
        to = {}
        for axis in range(2):
            for sign, by in (("+", 1), ("-", -1)):
                to["AB"[axis] + sign] = (axis, by, move(names[axis], at[axis], by))
        ways.append((h, n, to))

    def piece(way, da, db, which):
        h, n, _ = way
        da, db = da % n[0], db % n[1]
        ref = xs.at[place[(da, db) if h else (db, da)], h]
        return {0: ref, 1: ref.at[0:half], 2: ref.at[half:sat_n]}[which]

    def go(way, name, da, db, which):
        axis, by, to = way[2][name]
        there = (da - by, db) if axis == 0 else (da, db - by)
        copies.start(
            (way[0], name, da, db, which),
            lambda: piece(way, da, db, which),
            lambda: piece(way, *there, which),
            to,
        )

    def got(way, name, da, db, which):
        copies.arrive((way[0], name, da, db, which))

    def codes():
        copies.arrive("rep")

    def own():
        mine.wait()
        for k in range(len(peers)):
            copies.arrive(("sat", k))
        for way in ways:
            for name in ("A+", "A-", "B+", "B-"):
                go(way, name, 0, 0, 0)

    def first():
        for way in ways:
            got(way, "A+", 0, 0, 0)
            go(way, "A+", -1, 0, 1)
            got(way, "A-", 0, 0, 0)
            go(way, "A-", 1, 0, 2)
        for way in ways:
            got(way, "B+", 0, 0, 0)
            got(way, "B-", 0, 0, 0)
        for way in ways:
            for da in (-1, 1):
                go(way, "B+", da, 0, 0)
                go(way, "B-", da, 0, 0)
        for way in ways:
            go(way, "B+", 0, -1, 1)
            go(way, "B-", 0, 1, 2)

    def second():
        for way in ways:
            got(way, "A+", -1, 0, 1)
            got(way, "A-", 1, 0, 2)
            for name in ("B+", "B-"):
                go(way, name, 2, 0, 1)
                go(way, name, 2, 0, 2)

    def third():
        for way in ways:
            for da in (-1, 1):
                got(way, "B+", da, 0, 0)
                go(way, "B+", da, -1, 1)
                got(way, "B-", da, 0, 0)
                go(way, "B-", da, 1, 2)

    def fourth():
        for way in ways:
            for which in (1, 2):
                got(way, "B+", 2, 0, which)
                got(way, "B-", 2, 0, which)
            go(way, "B+", 2, -1, 1)
            go(way, "B-", 2, 1, 2)
            for da in (0, -1, 1):
                got(way, "B+", da, -1, 1)
                got(way, "B-", da, 1, 2)

    def fifth():
        for way in ways:
            got(way, "B+", 2, -1, 1)
            got(way, "B-", 2, 1, 2)

    hooks = {
        "codes": codes,
        "own": own,
        "first": first,
        "stages": {3: second, 4: third, 8: fourth, 11: fifth},
    }

    def run(*accs):
        energy = search(hooks, xs, ph, (rep, rep2), *tables, part, cs, ys, zs, accs)
        stat[...] = jnp.broadcast_to(jnp.sum(energy), (8, INNER))

    pl.run_scoped(run, *search_kinds())

    for s in range(sats):
        copies.start(("part", s), lambda s=s: part.at[sats + s], lambda s=s: land.at[s], partner)
    copies.start("stat", lambda: stat, lambda: stat2, partner)
    tops = []
    for s in range(sats):
        copies.arrive(("part", s))
        top = None
        for f in range(bins):
            v = part[s, f] + land[s, f]
            out[s, pl.ds(f, OUTER, stride=bins), :] = v
            top = v if top is None else jnp.maximum(top, v)
        tops.append(jnp.broadcast_to(jnp.max(top), (1, INNER)))
    tops.append(jnp.zeros((8 - sats, INNER), f32))
    copies.arrive("stat")
    mean = (stat[...] + stat2[...]) * (1.0 / (BLOCKS * LENGTH))
    best = jnp.concatenate(tops, 0) / jnp.maximum(mean, 0.25)
    peak[...] = best
    for k, to in enumerate(others):
        copies.start(("peak", k), lambda: peak, lambda k=k: peak2.at[k], to)
    for k in range(len(others)):
        copies.arrive(("peak", k))
        best = jnp.maximum(best, peak2[k])
    det[...] = best
    copies.drain()


def whole_call(x, rep, turns, sizes):
    sats = rep.shape[0]
    tm_n = sizes[TM[0]] * sizes[TM[1]]
    sat_n = sizes[SAT[0]] * sizes[SAT[1]]
    tables = [jnp.asarray(t) for t in dft_tables()]
    bins = turns.shape[0] // tm_n
    sems = sat_n + 44 + sats + tm_n
    return pl.pallas_call(
        functools.partial(whole, sizes),
        out_shape=(
            jax.ShapeDtypeStruct((sats, OUTER * bins, INNER), f32),
            jax.ShapeDtypeStruct((8, INNER), f32),
        ),
        in_specs=[VM, VM, pl.BlockSpec(memory_space=pltpu.SMEM)]
        + [VM] * len(tables),
        out_specs=(VM, VM),
        scratch_shapes=[
            pltpu.VMEM((bins, 2, OUTER, INNER), f32),
            pltpu.VMEM((tm_n, 2, sat_n, *x.shape[2:]), x.dtype),
            pltpu.VMEM(rep.shape, f32),
            pltpu.VMEM((2 * sats, bins, OUTER, INNER), f32),
            pltpu.VMEM((2 * sats, 2, OUTER, INNER), f32),
            pltpu.VMEM((2, bins, 2, OUTER, INNER), f32),
            pltpu.VMEM((2, 4, 2, OUTER, INNER), bf16),
            pltpu.VMEM((sats, bins, OUTER, INNER), f32),
            pltpu.VMEM((8, INNER), f32),
            pltpu.VMEM((8, INNER), f32),
            pltpu.VMEM((8, INNER), f32),
            pltpu.VMEM((tm_n - 1, 8, INNER), f32),
            pltpu.SemaphoreType.DMA((sems,)),
            pltpu.SemaphoreType.DMA((sems,)),
            pltpu.SemaphoreType.DMA((1,)),
        ],
        compiler_params=pltpu.CompilerParams(
            collective_id=1,
            has_side_effects=True,
            vmem_limit_bytes=32 * 2**20,
        ),
    )(x, rep, turns, *tables)


def replica_rows(codes):
    sats, chips = codes.shape
    assert (chips, LENGTH) == (CHIPS, 8192)
    c = codes.reshape(sats, 4, 1023).astype(bf16)
    even = jnp.concatenate([c[..., :1], c], -1)
    odd = jnp.concatenate([c[..., :512], c[..., 511:]], -1)
    h = lax.broadcasted_iota(jnp.int32, even.shape, 2)
    even = jnp.where((h > 0) & (h <= 512), -even, even)
    odd = jnp.where(h >= 512, -odd, odd)
    r = lax.broadcasted_iota(jnp.int32, (2 * INNER, 2 * INNER), 0)
    j = lax.broadcasted_iota(jnp.int32, (2 * INNER, 2 * INNER), 1)
    spread = (j == 2 * (r % INNER) + r // INNER).astype(bf16)
    both = jnp.concatenate([even.reshape(-1, INNER), odd.reshape(-1, INNER)], 1)
    rows = jnp.dot(both, spread, preferred_element_type=f32)
    return rows.reshape(sats, OUTER, INNER)


def shards(samples, codes, dopplers):
    sizes = {a: lax.axis_size(a) for a in (*TM, *SAT)}
    tm_n = sizes[TM[0]] * sizes[TM[1]]
    bins = dopplers.shape[0] // tm_n
    sats = codes.shape[0]
    x = samples.reshape(2, samples.shape[1], -1, INNER)
    rep = replica_rows(codes)
    power, det = whole_call(x, rep, dopplers, sizes)
    power = power.reshape(sats, OUTER, bins, INNER).transpose(2, 0, 1, 3)
    return power.reshape(bins, sats, LENGTH), det[:sats, 0]


def solution(mesh):
    torus = Mesh(mesh.devices.reshape(4, 4, 8, 2), (*TM, *SAT))
    body = jax.shard_map(
        shards,
        mesh=torus,
        in_specs=(P(None, TM, SAT), P(SAT, None), P()),
        out_specs=(P(TM, SAT, None), P(SAT)),
        check_vma=False,
    )
    with jax.sharding.use_abstract_mesh(torus.abstract_mesh):
        return body
```

```python
import functools
import math

import jax
import jax.numpy as jnp
import numpy as np
from jax import lax
from jax.experimental import pallas as pl
from jax.experimental.pallas import tpu as pltpu
from jax.sharding import Mesh
from jax.sharding import PartitionSpec as P

SAT = ("sat_0", "sat_1")
TM = ("tm_0", "tm_1")
MESH_ID = pl.DeviceIdType.MESH

OUTER = 64
INNER = 128
LENGTH = OUTER * INNER
CHIPS = 4092
BLOCKS = 32
SAMPLE_SCALE = 2.0**-29
WRAP = 32768
CORR_SCALE = 2.0**-22

f32 = jnp.float32
bf16 = jnp.bfloat16


def np_split(w):
    hi = w.astype(np.float32).astype(bf16)
    lo = (w - hi.astype(np.float64)).astype(np.float32).astype(bf16)
    return hi, lo


def halves(t):
    return np.stack([t[:, :INNER], t[:, INNER:]])


def dft_tables():
    i = np.arange(OUTER)
    a = 2 * np.pi * ((i[:, None] * i[None, :]) % OUTER) / OUTER
    c, s = np.cos(a), np.sin(a)
    rows = np.concatenate([k + np.arange(8 * b, 8 * b + 8) for b in range(8) for k in (0, 64)])
    cols = np.concatenate(
        [k + np.arange(16 * b, 16 * b + 16) for b in range(4) for k in (0, 128, 64, 192)]
    )

    def left(w):
        hi, lo = np_split(w)
        top = np.block([hi, hi])[rows]
        low = np.block([lo, np.zeros_like(lo)])[rows]
        return halves(np.concatenate([top, low])[:, cols])

    j = np.arange(INNER)
    b = 2 * np.pi * ((j[:, None] * j[None, :]) % INNER) / INNER
    ci, si = np.cos(b), np.sin(b)
    right = [np.block([[ci, -si], [si, ci]]), np.block([[ci, si], [-si, ci]])]
    t = 2 * np.pi * (i[:, None] * j[None, :]) / LENGTH
    return (
        left(np.block([[c, s], [-s, c]])),
        left(np.block([[c, -s], [s, c]])),
        *[halves(m) for r in right for m in np_split(r)],
        np.stack([np.cos(t), np.sin(t)]).astype(np.float32),
    )


def split(v):
    hi = v.astype(bf16)
    return hi, (v - hi.astype(f32)).astype(bf16)


def wide(ref, a, b):
    return jnp.concatenate([ref[0, a:b, :], ref[1, a:b, :]], 1)


def search_kinds():
    kinds = []
    for q in range(2):
        kinds += [pltpu.ACC(q)((OUTER, 256), f32)] * 8 + [pltpu.ACC(q)((128, 256), f32)] * 4
    return kinds


def search(hooks, xs, ph, reps, lf, li, rfh, rfl, rih, ril, tw, out, cs, ys, zs, accs):
    blocks = xs.shape[0]
    sats, bins = out.shape[:2]
    assert (sats, bins) == (6, 4)
    rep = lambda s: reps[s // 3][s % 3]
    if True:
        lag_acc = [accs[0:8], accs[12:20]]
        pair_acc = [accs[8:12], accs[20:24]]

        def tile(pairs):
            pieces = []
            for c in range(4):
                got = [[split(v[16 * c : 16 * c + 16]) for v in p] for p in pairs]
                for part in range(2):
                    for prec in range(2):
                        pieces.append(jnp.concatenate([g[part][prec] for g in got], 1))
            return jnp.concatenate(pieces, 0)

        def outer_start(q, k, left, pairs):
            pltpu.matmul_push_rhs(tile(pairs), 0, q)
            pltpu.matmul_acc_lhs(pair_acc[q][k], wide(left, 0, 128), load_staged_rhs=0)
            pltpu.matmul_acc_lhs(pair_acc[q][k], wide(left, 128, 256))

        def outer_end(q, k):
            o = pltpu.matmul_pop(pair_acc[q][k])
            got = []
            for u in range(2):
                v = o[:, INNER * u : INNER * u + INNER]
                got.append(
                    tuple(
                        jnp.concatenate([v[16 * c + d : 16 * c + d + 8] for c in range(8)], 0)
                        for d in (0, 8)
                    )
                )
            return got

        def forward_inner(q):
            tc, ts = tw[0], tw[1]
            v = [
                jnp.concatenate([r * tc + i * ts, i * tc - r * ts], 1)
                for r, i in outer_end(q, 3)
            ]
            hi, lo = split(jnp.concatenate(v, 0))
            pltpu.matmul_push_rhs(wide(rfh, 0, 256), 1, q)
            pltpu.matmul_acc_lhs(pair_acc[q][3], hi, load_staged_rhs=1)
            pltpu.matmul_acc_lhs(pair_acc[q][3], lo)
            pltpu.matmul_push_rhs(wide(rfl, 0, 256), 0, q)
            pltpu.matmul_acc_lhs(pair_acc[q][3], hi, load_staged_rhs=0)

        def forward_end(q):
            o = pltpu.matmul_pop(pair_acc[q][3])
            return [(o[64 * j : 64 * j + 64, :128], o[64 * j : 64 * j + 64, 128:]) for j in range(2)]

        for acc in accs:
            pltpu.matmul_pop(acc)
        hooks["codes"]()
        zero = jnp.zeros((OUTER, INNER), f32)
        for base in (0, 2):
            use = [[base + 2 * q, base + 2 * q + 1] for q in range(2)]
            for q in range(2):
                outer_start(q, 3, lf, [(rep(s), zero) for s in use[q]])
            for q in range(2):
                forward_inner(q)
            for q in range(2):
                for s, (r, i) in zip(use[q], forward_end(q)):
                    cs[s, 0] = r * CORR_SCALE
                    cs[s, 1] = i * CORR_SCALE
        out[...] = jnp.zeros_like(out)

        def signal(b):
            return [xs[b, h].reshape(OUTER, INNER).astype(f32) * SAMPLE_SCALE for h in range(2)]

        def forward_outer(q, x):
            turned = []
            for f in (2 * q, 2 * q + 1):
                c, s = ph[f, 0], ph[f, 1]
                turned.append((x[0] * c + x[1] * s, x[1] * c - x[0] * s))
            outer_start(q, 3, lf, turned)

        def forward_store(q, slot):
            for j, (r, i) in enumerate(forward_end(q)):
                ys[slot, 2 * q + j, 0] = r
                ys[slot, 2 * q + j, 1] = i

        def unit(u):
            return u % sats, u // sats

        def inverse_inner(q, slot, u):
            s, second = unit(u)
            f = 2 * q + second
            if u % 4 == 0:
                pltpu.matmul_push_rhs(wide(rih, 0, 256), 1, q)
            yr, yi = ys[slot, f, 0], ys[slot, f, 1]
            cr, ci = cs[s, 0], cs[s, 1]
            hi, lo = split(jnp.concatenate([yr * cr + yi * ci, yi * cr - yr * ci], 1))
            zs[q, u % 4, 0] = hi[:, :128]
            zs[q, u % 4, 1] = hi[:, 128:]
            acc = lag_acc[q][u % 8]
            pltpu.matmul_acc_lhs(acc, hi, load_staged_rhs=1 if u % 4 == 0 else None)
            pltpu.matmul_acc_lhs(acc, lo)

        def inverse_inner_low(q, group):
            pltpu.matmul_push_rhs(wide(ril, 0, 256), 0, q)
            for u in range(4 * group, 4 * group + 4):
                pltpu.matmul_acc_lhs(
                    lag_acc[q][u % 8],
                    wide(zs.at[q, u % 4], 0, OUTER),
                    load_staged_rhs=0 if u % 4 == 0 else None,
                )

        def inverse_outer(q, p):
            tc, ts = tw[0], tw[1]
            pairs = []
            for u in (2 * p, 2 * p + 1):
                o = pltpu.matmul_pop(lag_acc[q][u % 8])
                r, i = o[:, :128], o[:, 128:]
                pairs.append((r * tc - i * ts, i * tc + r * ts))
            outer_start(q, p % 3, li, pairs)

        def inverse_power(q, p):
            for u, (r, i) in zip((2 * p, 2 * p + 1), outer_end(q, p % 3)):
                s, second = unit(u)
                out[s, 2 * q + second] += r * r + i * i

        part = functools.partial

        def group_steps(q, slot, group):
            steps = [(64, part(inverse_inner, q, slot, u)) for u in range(4 * group, 4 * group + 4)]
            return steps + [(128, part(inverse_inner_low, q, group))]

        def pair_steps(q, p):
            return [(128, part(inverse_outer, q, p)), (0, part(inverse_power, q, (p - 2) % 6))]

        def early(q, slot, x):
            ahead = x is not None
            return [
                *([(128, part(forward_outer, q, x))] if ahead else []),
                *group_steps(q, slot, 0),
                *([(192, part(forward_inner, q))] if ahead else []),
                *group_steps(q, slot, 1),
                *pair_steps(q, 0),
                *pair_steps(q, 1),
            ]

        def late(q, slot, ahead=True):
            return [
                *group_steps(q, slot, 2),
                *([(0, part(forward_store, q, 1 - slot))] if ahead else []),
                *[step for p in range(2, 6) for step in pair_steps(q, p)],
            ]

        def merged(streams):
            at = [0, 0]
            todo = [list(v) for v in streams]
            while any(todo):
                q = min((at[q], q) for q in range(2) if todo[q])[1]
                cost, step = todo[q].pop(0)
                step()
                at[q] += cost

        def forward(b):
            x = signal(b)
            for q in range(2):
                forward_outer(q, x)
            for q in range(2):
                forward_inner(q)
            return x[0] * x[0] + x[1] * x[1]

        hooks["own"]()
        energy = forward(0)
        for q in range(2):
            forward_store(q, 0)
        merged([early(0, 0, None) + late(0, 0, False), early(1, 0, None)])
        hooks["first"]()
        energy = energy + forward(1)
        forward_store(0, 1)

        def body(b, energy):
            for k, stage in hooks["stages"].items():
                pl.when(b == k)(stage)
            slot = lax.rem(b, 2)
            x = signal(jnp.minimum(b + 1, blocks - 1))
            merged([early(0, slot, x) + late(0, slot), late(1, 1 - slot) + early(1, slot, x)])
            return energy + jnp.where(b + 1 < blocks, x[0] * x[0] + x[1] * x[1], 0.0)

        energy = lax.fori_loop(1, blocks, body, energy)
        for p in (4, 5):
            inverse_power(0, p)
        hooks["half"](0)
        merged([[], late(1, (blocks - 1) % 2)])
        for p in (4, 5):
            inverse_power(1, p)
        return energy


VM = pl.BlockSpec(memory_space=pltpu.VMEM)


class Copies:
    def __init__(self, send, recv):
        self.send, self.recv, self.made = send, recv, {}

    def make(self, key):
        n, src, dst, to = self.made[key]
        return pltpu.make_async_remote_copy(
            src_ref=src(),
            dst_ref=dst(),
            send_sem=self.send.at[n],
            recv_sem=self.recv.at[n],
            device_id=to,
            device_id_type=MESH_ID,
        )

    def start(self, key, src, dst, to):
        self.made[key] = (len(self.made), src, dst, to)
        self.make(key).start()

    def arrive(self, key):
        self.make(key).wait_recv()

    def drain(self):
        for key in self.made:
            self.make(key).wait_send()


def phasors(turns, start, ph):
    shape = ph.shape[2:]
    n = lax.broadcasted_iota(jnp.int32, shape, 0) * INNER + lax.broadcasted_iota(jnp.int32, shape, 1)
    for f in range(ph.shape[0]):
        m = (turns[start + f] * n) & (WRAP - 1)
        quarter = (m + WRAP // 8) >> 13
        t = (m - (quarter << 13)).astype(f32) * (2.0 * math.pi / WRAP)
        u = t * t
        sine = t * (1 + u * (-1 / 6 + u * (1 / 120 + u * (-1 / 5040 + u * (1 / 362880)))))
        cosine = 1 + u * (
            -1 / 2 + u * (1 / 24 + u * (-1 / 720 + u * (1 / 40320 + u * (-1 / 3628800))))
        )
        odd, half = (quarter & 1) == 1, (quarter & 2) == 2
        c = jnp.where(odd, -sine, cosine)
        s = jnp.where(odd, cosine, sine)
        ph[f, 0] = jnp.where(half, -c, c)
        ph[f, 1] = jnp.where(half, -s, s)


def positions(ny, nx):
    far = lambda d, n: min(d, n - d)
    order = sorted(
        ((dy, dx) for dy in range(ny) for dx in range(nx)),
        key=lambda o: (far(o[0], ny) + far(o[1], nx), max(far(o[0], ny), far(o[1], nx)), o),
    )
    return {o: p for p, o in enumerate(order)}


def whole(sizes, x, rep, bins_ref, *refs):
    tables, out, det, ph, refs = refs[:7], refs[7], refs[8], refs[9], refs[10:]
    xs, rep2, part, cs, ys, zs, land, stat, stat2, peak, peak2, send, recv, local = refs
    y, xx, z, core = (lax.axis_index(a) for a in (*TM, *SAT))
    ny, nx, nz, nc = (sizes[a] for a in (*TM, *SAT))
    sat, sat_n = z * nc + core, nz * nc
    tm, tm_n = y * nx + xx, ny * nx
    sats, bins = land.shape[:2]
    move = lambda axis, at, by: {axis: lax.rem(at + by + sizes[axis], sizes[axis])}
    peers = []
    for k in sorted(range(1, sat_n), key=lambda k: -min(k, sat_n - k)):
        t = lax.rem(sat + k, sat_n)
        peers.append((t % nc, {SAT[0]: t // nc, SAT[1]: t % nc}))
    others = []
    ring = lambda d, n: min(d, n - d)
    for dy, dx in sorted(
        ((dy, dx) for dy in range(ny) for dx in range(nx) if dy or dx),
        key=lambda o: (-ring(o[0], ny) - ring(o[1], nx), o),
    ):
        others.append({**move(TM[0], y, dy), **move(TM[1], xx, dx)})
    partner = {SAT[1]: 1 - core}
    barrier = pltpu.get_barrier_semaphore()
    greeted = [to for _, to in peers] + others
    for to in greeted:
        pl.semaphore_signal(barrier, inc=1, device_id=to, device_id_type=MESH_ID)
    phasors(bins_ref, tm * bins, ph)
    pl.semaphore_wait(barrier, len(greeted))

    copies = Copies(send, recv)
    for k, (block, to) in enumerate(peers):
        copies.start(("sat", k), lambda b=block: x.at[:, b], lambda: xs.at[0, :, sat], to)
    copies.start("rep", lambda: rep, lambda: rep2, partner)
    mine = pltpu.make_async_copy(x.at[:, core], xs.at[0, :, sat], local.at[0])
    mine.start()

    place = positions(ny, nx)
    half = sat_n // 2
    ways = []
    for h in range(2):
        names, at, n = ((TM[1], TM[0]), (xx, y), (nx, ny))
        if h:
            names, at, n = names[::-1], at[::-1], n[::-1]
        to = {}
        for axis in range(2):
            for sign, by in (("+", 1), ("-", -1)):
                to["AB"[axis] + sign] = (axis, by, move(names[axis], at[axis], by))
        ways.append((h, n, to))

    def piece(way, da, db, which):
        h, n, _ = way
        da, db = da % n[0], db % n[1]
        ref = xs.at[place[(da, db) if h else (db, da)], h]
        return {0: ref, 1: ref.at[0:half], 2: ref.at[half:sat_n]}[which]

    def go(way, name, da, db, which):
        axis, by, to = way[2][name]
        there = (da - by, db) if axis == 0 else (da, db - by)
        copies.start(
            (way[0], name, da, db, which),
            lambda: piece(way, da, db, which),
            lambda: piece(way, *there, which),
            to,
        )

    def got(way, name, da, db, which):
        copies.arrive((way[0], name, da, db, which))

    def codes():
        copies.arrive("rep")

    def own():
        mine.wait()
        for k in range(len(peers)):
            copies.arrive(("sat", k))
        for way in ways:
            for name in ("A+", "A-", "B+", "B-"):
                go(way, name, 0, 0, 0)

    def first():
        for way in ways:
            got(way, "A+", 0, 0, 0)
            go(way, "A+", -1, 0, 1)
            got(way, "A-", 0, 0, 0)
            go(way, "A-", 1, 0, 2)
        for way in ways:
            got(way, "B+", 0, 0, 0)
            got(way, "B-", 0, 0, 0)
        for way in ways:
            for da in (-1, 1):
                go(way, "B+", da, 0, 0)
                go(way, "B-", da, 0, 0)
        for way in ways:
            go(way, "B+", 0, -1, 1)
            go(way, "B-", 0, 1, 2)

    def second():
        for way in ways:
            got(way, "A+", -1, 0, 1)
            got(way, "A-", 1, 0, 2)
            for name in ("B+", "B-"):
                go(way, name, 2, 0, 1)
                go(way, name, 2, 0, 2)

    def third():
        for way in ways:
            for da in (-1, 1):
                got(way, "B+", da, 0, 0)
                go(way, "B+", da, -1, 1)
                got(way, "B-", da, 0, 0)
                go(way, "B-", da, 1, 2)

    def fourth():
        for way in ways:
            for which in (1, 2):
                got(way, "B+", 2, 0, which)
                got(way, "B-", 2, 0, which)
            go(way, "B+", 2, -1, 1)
            go(way, "B-", 2, 1, 2)
            for da in (0, -1, 1):
                got(way, "B+", da, -1, 1)
                got(way, "B-", da, 1, 2)

    def fifth():
        for way in ways:
            got(way, "B+", 2, -1, 1)
            got(way, "B-", 2, 1, 2)

    pairs = bins // 2

    def swap(half):
        for s in range(sats):
            copies.start(
                ("part", s, half),
                lambda s=s: part.at[sats + s, half * pairs : half * pairs + pairs],
                lambda s=s: land.at[s, half * pairs : half * pairs + pairs],
                partner,
            )

    hooks = {
        "half": swap,
        "codes": codes,
        "own": own,
        "first": first,
        "stages": {3: second, 4: third, 8: fourth, 11: fifth},
    }

    def run(*accs):
        energy = search(hooks, xs, ph, (rep, rep2), *tables, part, cs, ys, zs, accs)
        stat[...] = jnp.broadcast_to(jnp.sum(energy), (8, INNER))

    pl.run_scoped(run, *search_kinds())

    swap(1)
    copies.start("stat", lambda: stat, lambda: stat2, partner)
    tops = []
    for s in range(sats):
        top = None
        for f in range(bins):
            if f % pairs == 0:
                copies.arrive(("part", s, f // pairs))
            v = part[s, f] + land[s, f]
            out[s, pl.ds(f, OUTER, stride=bins), :] = v
            top = v if top is None else jnp.maximum(top, v)
        tops.append(jnp.broadcast_to(jnp.max(top), (1, INNER)))
    tops.append(jnp.zeros((8 - sats, INNER), f32))
    copies.arrive("stat")
    mean = (stat[...] + stat2[...]) * (1.0 / (BLOCKS * LENGTH))
    best = jnp.concatenate(tops, 0) / jnp.maximum(mean, 0.25)
    peak[...] = best
    for k, to in enumerate(others):
        copies.start(("peak", k), lambda: peak, lambda k=k: peak2.at[k], to)
    for k in range(len(others)):
        copies.arrive(("peak", k))
        best = jnp.maximum(best, peak2[k])
    for s in range(sats):
        det[s] = jnp.max(best[s : s + 1])
    copies.drain()


def whole_call(x, rep, turns, sizes):
    sats = rep.shape[0]
    tm_n = sizes[TM[0]] * sizes[TM[1]]
    sat_n = sizes[SAT[0]] * sizes[SAT[1]]
    tables = [jnp.asarray(t) for t in dft_tables()]
    bins = turns.shape[0] // tm_n
    sems = sat_n + 44 + 2 * sats + tm_n
    return pl.pallas_call(
        functools.partial(whole, sizes),
        out_shape=(
            jax.ShapeDtypeStruct((sats, OUTER * bins, INNER), f32),
            jax.ShapeDtypeStruct((sats,), f32),
        ),
        in_specs=[VM, VM, pl.BlockSpec(memory_space=pltpu.SMEM)]
        + [VM] * len(tables),
        out_specs=(VM, pl.BlockSpec(memory_space=pltpu.SMEM)),
        scratch_shapes=[
            pltpu.VMEM((bins, 2, OUTER, INNER), f32),
            pltpu.VMEM((tm_n, 2, sat_n, *x.shape[2:]), x.dtype),
            pltpu.VMEM(rep.shape, f32),
            pltpu.VMEM((2 * sats, bins, OUTER, INNER), f32),
            pltpu.VMEM((2 * sats, 2, OUTER, INNER), f32),
            pltpu.VMEM((2, bins, 2, OUTER, INNER), f32),
            pltpu.VMEM((2, 4, 2, OUTER, INNER), bf16),
            pltpu.VMEM((sats, bins, OUTER, INNER), f32),
            pltpu.VMEM((8, INNER), f32),
            pltpu.VMEM((8, INNER), f32),
            pltpu.VMEM((8, INNER), f32),
            pltpu.VMEM((tm_n - 1, 8, INNER), f32),
            pltpu.SemaphoreType.DMA((sems,)),
            pltpu.SemaphoreType.DMA((sems,)),
            pltpu.SemaphoreType.DMA((1,)),
        ],
        compiler_params=pltpu.CompilerParams(
            collective_id=1,
            has_side_effects=True,
            vmem_limit_bytes=32 * 2**20,
        ),
    )(x, rep, turns, *tables)


def replica_rows(codes):
    sats, chips = codes.shape
    assert (chips, LENGTH) == (CHIPS, 8192)
    c = codes.reshape(sats, 4, 1023).astype(bf16)
    even = jnp.concatenate([c[..., :1], c], -1)
    odd = jnp.concatenate([c[..., :512], c[..., 511:]], -1)
    h = lax.broadcasted_iota(jnp.int32, even.shape, 2)
    even = jnp.where((h > 0) & (h <= 512), -even, even)
    odd = jnp.where(h >= 512, -odd, odd)
    r = lax.broadcasted_iota(jnp.int32, (2 * INNER, 2 * INNER), 0)
    j = lax.broadcasted_iota(jnp.int32, (2 * INNER, 2 * INNER), 1)
    spread = (j == 2 * (r % INNER) + r // INNER).astype(bf16)
    both = jnp.concatenate([even.reshape(-1, INNER), odd.reshape(-1, INNER)], 1)
    rows = jnp.dot(both, spread, preferred_element_type=f32)
    return rows.reshape(sats, OUTER, INNER)


def shards(samples, codes, dopplers):
    sizes = {a: lax.axis_size(a) for a in (*TM, *SAT)}
    tm_n = sizes[TM[0]] * sizes[TM[1]]
    bins = dopplers.shape[0] // tm_n
    sats = codes.shape[0]
    x = samples.reshape(2, samples.shape[1], -1, INNER)
    rep = replica_rows(codes)
    power, det = whole_call(x, rep, dopplers, sizes)
    power = power.reshape(sats, OUTER, bins, INNER).transpose(2, 0, 1, 3)
    return power.reshape(bins, sats, LENGTH), det


def solution(mesh):
    torus = Mesh(mesh.devices.reshape(4, 4, 8, 2), (*TM, *SAT))
    body = jax.shard_map(
        shards,
        mesh=torus,
        in_specs=(P(None, TM, SAT), P(SAT, None), P()),
        out_specs=(P(TM, SAT, None), P(SAT)),
        check_vma=False,
    )
    with jax.sharding.use_abstract_mesh(torus.abstract_mesh):
        return body
```
